512 devices in a mesh: seq: 32 (over x_hi, z), head: 16 (over x_lo, y, core).
Axes of the slice: x: 4 (x_hi: 2, x_lo: 2; x = x_hi * 2 + x_lo), y: 4, z: 16, core: 2. Of those that a mesh axis runs over, the one named last changes fastest.
Arguments:
- tokens: bfloat16 [8192, 4608], P('seq', 'head'), may hold values from -32 to 32
- segments: int32 [8192], P('seq'), may hold values from 0 to 7, never falling along the last dimension, each value on 1 to 4096 neighbouring positions
- pre_gain: float32 [4608], replicated, may hold values from 0.1 to 1.9
- post_gain: float32 [4608], replicated, may hold values from 0.1 to 1.9
- w_query: bfloat16 [4608, 4096], P('seq', 'head'), may hold values from -0.375 to 0.375
- w_key: bfloat16 [4608, 2048], P('seq', 'head'), may hold values from -0.1875 to 0.1875
- w_value: bfloat16 [4608, 2048], P('seq', 'head'), may hold values from -0.09375 to 0.09375
- w_out: bfloat16 [4096, 4608], P('head', 'seq'), may hold values from -0.09375 to 0.09375
Outputs:
- mixed: bfloat16 [8192, 4608], P('seq')
The draws below stay inside these ranges and needn't reach their ends.
Inputs may be any that keep to these rules, and one draw needn't show every extreme that they name: `segments`: segment ids never fall; each of the 8 documents holds at least one token and at most 4096, one exactly 4096.
All inputs are finite; a program needn't handle non-finite values.
Results may differ from the reference program's by a relative error of at most 0.01.
Values may be sent and summed in bfloat16 or wider, within the bound.
No kernel may reach another device: no remote copies, remote signals or barrier semaphores. Data moves between devices by JAX's collectives and lax.ppermute only.
A program may use at most 64 MiB of HBM per device.

```python
import math
import jax
import jax.numpy as jnp
import numpy as np
from jax import lax

D = 4608
HD = 128
GROUP = 2
SCALAR = 144
DOCS = 8
KV_HEADS = 16
HEADS = 32
TOKENS = 8192
MOST = 4096
N_HEAD = 16


def draw_tokens(key, part):
    first, second, third = jax.random.split(jax.random.fold_in(key, 11), 3)
    base = jnp.clip(jax.random.normal(first, (TOKENS, D), jnp.float32), -4.0, 4.0)
    rows = jnp.exp(jax.random.uniform(second, (TOKENS, 1), jnp.float32, jnp.log(0.3), jnp.log(3.0)))
    cols = jnp.exp(jax.random.uniform(third, (1, D), jnp.float32, jnp.log(0.3), jnp.log(3.0)))
    return jnp.clip(base * rows * cols, -32.0, 32.0).astype(jnp.bfloat16)


def block_scale(rng, dims, pieces, least, high):
    level, own = 1.0, jax.random.fold_in(rng, 6)
    for axis_at, blocks in pieces:
        draws = jnp.exp(jax.random.uniform(jax.random.fold_in(own, axis_at), (blocks,), jnp.float32, least / len(pieces), high / len(pieces)))
        level = level * jnp.repeat(draws, dims[axis_at] // blocks).reshape([-1 if axis == axis_at else 1 for axis in range(len(dims))])
    return level


def profile(number_of, total, reach, lean):
    loads = [(1 << 20) // math.isqrt(grade ** lean) + 1 for grade in range(2, number_of + 1)]
    spare, given = total - reach - (number_of - 1), [1] * (number_of - 1)
    while spare > 0:
        free = [i for i in range(number_of - 1) if given[i] < reach]
        whole, budget = sum([loads[i] for i in free]), spare
        for i in free:
            extra = min(reach - given[i], max(1, budget * loads[i] // whole), spare)
            given[i] = given[i] + extra
            spare = spare - extra
    return np.array([reach] + given)


def ragged(rng, number_of, total, reach, lean):
    if number_of == 2:
        one = jax.random.randint(rng, (), max(1, total - reach), min(reach, total - 1) + 1)
        return jnp.stack([one, total - one])
    tallies = jnp.asarray(profile(number_of, total, reach, lean), jnp.int32)
    couples = (number_of - 1) // 2
    giver, taker = tallies[1:1 + 2 * couples:2], tallies[2:2 + 2 * couples:2]
    margin = jnp.minimum(giver - 1, reach - taker)
    passed = jax.random.randint(jax.random.fold_in(rng, 1), (couples,), 0, 1 << 20) % (margin + 1)
    tallies = tallies.at[1:1 + 2 * couples:2].set(giver - passed).at[2:2 + 2 * couples:2].set(taker + passed)
    return tallies[jax.random.permutation(jax.random.fold_in(rng, 2), number_of)]


def centred(own_key, dims, scale, limit, shards=(), held_as=jnp.bfloat16):
    values = jax.random.normal(own_key, dims, jnp.float32) * scale
    if len(shards) > 0:
        values = block_scale(own_key, dims, shards, -0.22, 0.18) * values
    return jnp.clip(values, min=-limit, max=limit).astype(held_as)


def setup_inputs(seed: int = 0) -> dict:
    key_list = jax.random.split(jax.random.key(seed), 9)
    return {
        "tokens": draw_tokens(jax.random.fold_in(key_list[8], 71), 0),
        "segments": jnp.searchsorted(jnp.cumsum(ragged(key_list[1], DOCS, TOKENS, MOST, 2)), jnp.arange(TOKENS), side="right").astype(jnp.int32),
        "pre_gain": jnp.clip(1.0 + 0.18 * jax.random.normal(key_list[2], (D,), jnp.float32), 0.1, 1.9),
        "post_gain": jnp.clip(1.0 + 0.18 * jax.random.normal(key_list[3], (D,), jnp.float32), 0.1, 1.9),
        "w_query": centred(key_list[4], (D, HEADS * HD), (D // 16) ** -0.5, 0.375, ((0, 32), (1, 16))),
        "w_key": centred(key_list[5], (D, KV_HEADS * HD), (D // 4) ** -0.5, 0.1875, ((0, 32), (1, 16))),
        "w_value": centred(key_list[6], (D, KV_HEADS * HD), D ** -0.5, 0.09375, ((0, 32), (1, 16))),
        "w_out": centred(key_list[7], (HEADS * HD, D), (HEADS * HD) ** -0.5, 0.09375, ((0, 16), (1, 32))),
    }


EPS = 1e-06
CAP = 50.0

def rotate(values, position, width):
    count = values.shape[1] // width
    half = width // 2
    shaped = values.reshape(values.shape[0], count, width)
    freq = 10000.0 ** (-(jnp.arange(half, dtype=jnp.float32) / half))
    angle = position[:, None] * freq[None, :]
    cosine = jnp.cos(angle)[:, None, :]
    sine = jnp.sin(angle)[:, None, :]
    first = shaped[:, :, :half]
    second = shaped[:, :, half:]
    turned = jnp.concatenate([first * cosine - second * sine, second * cosine + first * sine], axis=2)
    return turned.reshape(values.shape[0], count * width)

def reference(tokens, segments, pre_gain, post_gain, w_query, w_key, w_value, w_out):
    wide = tokens.astype(jnp.float32)
    normed = (wide * lax.rsqrt(lax.optimization_barrier(jnp.mean(wide * wide, axis=1, keepdims=True)) + EPS) * pre_gain).astype(jnp.bfloat16)
    query = jnp.dot(normed, w_query, preferred_element_type=jnp.float32)
    key_proj = jnp.dot(normed, w_key, preferred_element_type=jnp.float32)
    value_proj = jnp.dot(normed, w_value, preferred_element_type=jnp.float32)
    levels = jnp.arange(DOCS, dtype=jnp.int32)
    onehot = (segments[:, None] == levels[None, :]).astype(jnp.float32)
    counts = lax.optimization_barrier(jnp.sum(onehot, axis=0))
    before = jnp.cumsum(counts) - counts
    start = lax.optimization_barrier(jnp.sum(onehot * before[None, :], axis=1))
    index_f = jnp.arange(TOKENS, dtype=jnp.int32).astype(jnp.float32)
    position = index_f - start
    heads = HEADS
    kv_count = KV_HEADS
    rq = (rotate(query, position, HD) * SCALAR ** (-0.5)).astype(jnp.bfloat16)
    rq = rq.reshape(TOKENS, heads, HD).transpose(1, 0, 2)
    rk = rotate(key_proj, position, HD).astype(jnp.bfloat16).reshape(TOKENS, kv_count, HD).transpose(1, 0, 2)
    vb = value_proj.astype(jnp.bfloat16).reshape(TOKENS, kv_count, HD).transpose(1, 0, 2)
    allowed = (index_f[None, :] >= start[:, None]) & (index_f[None, :] <= index_f[:, None])

    def head_attn(head):
        qh = rq[head]
        kh = rk[head // GROUP]
        vh = vb[head // GROUP]
        scores = jnp.dot(qh, kh.T, preferred_element_type=jnp.float32)
        capped = CAP * jnp.tanh(scores / CAP)
        weights = jnp.where(allowed, jnp.exp(capped), 0.0)
        total = jnp.dot(weights.astype(jnp.bfloat16), vh, preferred_element_type=jnp.float32)
        return (total / lax.optimization_barrier(jnp.sum(weights, axis=1))[:, None]).astype(jnp.bfloat16)
    attn = lax.map(head_attn, jnp.arange(heads, dtype=jnp.int32))
    attn = attn.transpose(1, 0, 2).reshape(TOKENS, heads * HD)
    per = heads * HD // N_HEAD
    groups = attn.reshape(TOKENS, N_HEAD, per).transpose(1, 0, 2)
    out_groups = w_out.reshape(N_HEAD, per, D)

    def add_group(total, pair):
        part = jnp.dot(pair[0], pair[1], preferred_element_type=jnp.float32).astype(jnp.bfloat16)
        part = lax.optimization_barrier(part).astype(jnp.float32)
        return (total + part, None)
    proj, unused = lax.scan(add_group, jnp.zeros((TOKENS, D), jnp.float32), (groups, out_groups))
    scale = lax.rsqrt(lax.optimization_barrier(jnp.mean(proj * proj, axis=1, keepdims=True)) + EPS)
    return (wide + proj * scale * post_gain).astype(jnp.bfloat16)
```

```python
import jax
import jax.numpy as jnp
from jax import lax
from jax.experimental import pallas as pl
from jax.experimental.pallas import tpu as pltpu
from jax.sharding import Mesh
from jax.sharding import PartitionSpec as P

D = 4608
HD = 128
GROUP = 2
SCALAR = 144
DOCS = 8
SEQ = ("xh", "z")
HEAD = ("xl", "y", "c")
PLANE = ("xl", "y")

EPS = 1e-06
CAP = 50.0


def from_everyone(shard, axis):
    copies = jnp.broadcast_to(shard, (lax.axis_size(axis), *shard.shape))
    return lax.all_to_all(copies, axis, split_axis=0, concat_axis=0, tiled=True)


def rotate(values, cosine, sine):
    half = values.shape[1] // 2
    first = values[:, :half]
    second = values[:, half:]
    return jnp.concatenate(
        [first * cosine - second * sine, second * cosine + first * sine], axis=1
    )


def attend_kernel(where_ref, query_ref, start_ref, kv_hbm, out_ref, held, sums, total, sem):
    rows = query_ref.shape[0] // GROUP
    low = where_ref[0]
    own = where_ref[1]
    halves = where_ref[2]

    def fetch(j):
        place = (lax.rem(j, halves) * 2 + lax.div(j, halves)) * rows
        return pltpu.make_async_copy(
            kv_hbm.at[pl.ds(pl.multiple_of(place, rows), rows), :], held.at[j], sem.at[j]
        )

    @pl.loop(low, own + 1)
    def _(j):
        fetch(j).start()

    sums[...] = jnp.zeros_like(sums)
    total[...] = jnp.zeros_like(total)
    shape = (GROUP * rows, rows)
    row = lax.broadcasted_iota(jnp.int32, shape, 0)
    index = own * rows + jnp.where(row >= rows, row - rows, row)
    column = lax.broadcasted_iota(jnp.int32, shape, 1)

    @pl.loop(low, own + 1)
    def _(j):
        fetch(j).wait()
        keys = held[j, :, :HD]
        values = held[j, :, HD:]
        scores = lax.dot_general(
            query_ref[...], keys, (((1,), (1,)), ((), ())), preferred_element_type=jnp.float32
        )
        weights = jnp.exp(CAP * jnp.tanh(scores * (1.0 / CAP)))
        key_index = j * rows + column
        allowed = (key_index >= start_ref[...]) & (key_index <= index)
        weights = jnp.where(allowed, weights, 0.0)
        part = weights[:, :HD]
        for k in range(1, rows // HD):
            part = part + weights[:, k * HD : (k + 1) * HD]
        sums[...] += part
        total[...] += jnp.dot(
            weights.astype(jnp.bfloat16), values, preferred_element_type=jnp.float32
        )

    result = total[...] / jnp.sum(sums[...], axis=1, keepdims=True)
    for k in range(GROUP):
        out_ref[:, k * HD : (k + 1) * HD] = result[k * rows : (k + 1) * rows].astype(jnp.bfloat16)


def attend(where, stacked, starts, kv):
    rows = stacked.shape[0] // GROUP
    blocks = kv.shape[0] // rows
    vmem = pl.BlockSpec(memory_space=pltpu.VMEM)
    return pl.pallas_call(
        attend_kernel,
        out_shape=jax.ShapeDtypeStruct((rows, GROUP * HD), jnp.bfloat16),
        in_specs=[
            pl.BlockSpec(memory_space=pltpu.SMEM),
            vmem,
            vmem,
            pl.BlockSpec(memory_space=pl.ANY),
        ],
        out_specs=vmem,
        scratch_shapes=[
            pltpu.VMEM((blocks, rows, 2 * HD), jnp.bfloat16),
            pltpu.VMEM((GROUP * rows, HD), jnp.float32),
            pltpu.VMEM((GROUP * rows, HD), jnp.float32),
            pltpu.SemaphoreType.DMA((blocks,)),
        ],
        compiler_params=pltpu.CompilerParams(vmem_limit_bytes=24 * 1024 * 1024),
        cost_estimate=pl.CostEstimate(
            flops=4 * GROUP * rows * HD * kv.shape[0] // 2,
            bytes_accessed=kv.size,
            transcendentals=GROUP * rows * kv.shape[0],
        ),
    )(where, stacked, starts, kv)


def local(tokens, segments, pre_gain, post_gain, w_query, w_key, w_value, w_out):
    rows = tokens.shape[0]
    deep = lax.axis_size("z")
    slab = w_key.shape[0]
    mine = jnp.concatenate([w_key, w_value, w_query, w_out.T], axis=1)
    pair = lax.all_gather(mine, "xh", axis=0, tiled=True)
    weights = lax.all_gather(pair, "z", axis=0, tiled=True)

    whole = from_everyone(tokens.T, HEAD).reshape(D, rows)
    wide = whole.astype(jnp.float32)
    scale = lax.rsqrt(jnp.mean(wide * wide, axis=0, keepdims=True) + EPS)
    normed = (wide * scale * pre_gain[:, None]).astype(jnp.bfloat16)
    normed = normed.reshape(2, deep, slab, rows).transpose(1, 0, 2, 3).reshape(D, rows).T
    normed = lax.optimization_barrier(normed)

    levels = jnp.arange(DOCS, dtype=jnp.int32)
    counts = jnp.sum((levels[None, :] > segments[:, None]).astype(jnp.float32), axis=0)
    starts = jnp.sum(from_everyone(counts, SEQ).reshape(-1, DOCS), axis=0)
    onehot = (segments[:, None] == levels[None, :]).astype(jnp.float32)
    tok_start = jnp.sum(onehot * starts[None, :], axis=1)
    block = lax.axis_index(SEQ)
    index_f = (block * rows + jnp.arange(rows, dtype=jnp.int32)).astype(jnp.float32)
    position = index_f - tok_start
    half = HD // 2
    freq = 10000.0 ** (-(jnp.arange(half, dtype=jnp.float32) / half))
    angle = position[:, None] * freq[None, :]
    cosine, sine = jnp.cos(angle), jnp.sin(angle)
    start_i = tok_start.astype(jnp.int32)
    where = jnp.stack([start_i[0] // rows, block.astype(jnp.int32), jnp.int32(deep)])
    starts_col = jnp.tile(start_i, GROUP)[:, None]

    kv = jnp.dot(normed, weights[:, : 2 * HD], preferred_element_type=jnp.float32)
    rk = rotate(kv[:, :HD], cosine, sine).astype(jnp.bfloat16)
    vb = kv[:, HD:].astype(jnp.bfloat16)
    kv_pair = lax.all_gather(jnp.concatenate([rk, vb], axis=1), "xh", axis=0, tiled=True)
    kv_all = lax.all_gather(kv_pair, "z", axis=0, tiled=True)

    query = jnp.dot(normed, weights[:, 2 * HD : 4 * HD], preferred_element_type=jnp.float32)
    stacked = jnp.concatenate(
        [
            (rotate(query[:, k * HD : (k + 1) * HD], cosine, sine) * SCALAR ** (-0.5)).astype(
                jnp.bfloat16
            )
            for k in range(GROUP)
        ],
        axis=0,
    )
    out_t = weights[:, 4 * HD :].reshape(deep, 2, slab, GROUP * HD).transpose(1, 0, 2, 3)
    out_t = lax.optimization_barrier(out_t.reshape(D, GROUP * HD))

    near = lax.axis_size(PLANE)
    few = rows // (near * lax.axis_size("c"))
    first_row = (lax.axis_index("c") * near + lax.axis_index(PLANE)) * few
    own = lax.dynamic_slice_in_dim(whole, first_row, few, 1).T.astype(jnp.float32)

    attn = attend(where, stacked, starts_col, kv_all)
    partial = lax.dot_general(
        attn, out_t, (((1,), (1,)), ((), ())), preferred_element_type=jnp.float32
    ).astype(jnp.bfloat16)

    halves = lax.all_to_all(partial.reshape(2, rows // 2, D), "c", 0, 0, tiled=True)
    halves = (halves[0].astype(jnp.float32) + halves[1].astype(jnp.float32)).astype(jnp.bfloat16)
    pieces = lax.all_to_all(halves.reshape(near, few, D), PLANE, 0, 0, tiled=True)
    proj = jnp.sum(pieces.astype(jnp.float32), axis=0)
    post = lax.rsqrt(jnp.mean(proj * proj, axis=1, keepdims=True) + EPS)
    result = (own + proj * post * post_gain[None, :]).astype(jnp.bfloat16)
    result = from_everyone(result, PLANE).reshape(rows // 2, D)
    return from_everyone(result, "c").reshape(rows, D)


def solution(mesh):
    finer = Mesh(mesh.devices.reshape(2, 16, 2, 4, 2), ("xh", "z", "xl", "y", "c"))
    in_specs = (
        P(SEQ, HEAD),
        P(SEQ),
        P(),
        P(),
        P(SEQ, HEAD),
        P(SEQ, HEAD),
        P(SEQ, HEAD),
        P(HEAD, SEQ),
    )
    return jax.shard_map(
        local, mesh=finer, in_specs=in_specs, out_specs=P(SEQ, None), check_vma=False
    )
```

```python
import jax
import jax.numpy as jnp
from jax import lax
from jax.experimental import pallas as pl
from jax.experimental.pallas import tpu as pltpu
from jax.sharding import Mesh
from jax.sharding import PartitionSpec as P

D = 4608
HD = 128
GROUP = 2
SCALAR = 144
DOCS = 8
SEQ = ("xh", "z")
HEAD = ("xl", "y", "c")
PLANE = ("xl", "y")
WIDE = ("xh", "xl", "y")

EPS = 1e-06
CAP = 50.0


def from_everyone(shard, axis):
    copies = jnp.broadcast_to(shard, (lax.axis_size(axis), *shard.shape))
    return lax.all_to_all(copies, axis, split_axis=0, concat_axis=0, tiled=True)


def rotate(values, cosine, sine):
    half = values.shape[1] // 2
    first = values[:, :half]
    second = values[:, half:]
    return jnp.concatenate(
        [first * cosine - second * sine, second * cosine + first * sine], axis=1
    )


def attend_kernel(where_ref, query_ref, start_ref, kv_ref, out_ref, sums, total):
    rows = query_ref.shape[0] // GROUP
    low = where_ref[0]
    own = where_ref[1]
    half = kv_ref.shape[0] // (2 * rows)

    sums[...] = jnp.zeros_like(sums)
    total[...] = jnp.zeros_like(total)
    shape = (GROUP * rows, rows)
    row = lax.broadcasted_iota(jnp.int32, shape, 0)
    index = own * rows + jnp.where(row >= rows, row - rows, row)
    column = lax.broadcasted_iota(jnp.int32, shape, 1)

    @pl.loop(low, own + 1)
    def _(j):
        place = pl.multiple_of((lax.rem(j, 2) * half + lax.div(j, 2)) * rows, rows)
        keys = kv_ref[pl.ds(place, rows), :HD]
        values = kv_ref[pl.ds(place, rows), HD:]
        scores = lax.dot_general(
            query_ref[...], keys, (((1,), (1,)), ((), ())), preferred_element_type=jnp.float32
        )
        weights = jnp.exp(CAP * jnp.tanh(scores * (1.0 / CAP)))
        key_index = j * rows + column
        allowed = (key_index >= start_ref[...]) & (key_index <= index)
        weights = jnp.where(allowed, weights, 0.0)
        part = weights[:, :HD]
        for k in range(1, rows // HD):
            part = part + weights[:, k * HD : (k + 1) * HD]
        sums[...] += part
        total[...] += jnp.dot(
            weights.astype(jnp.bfloat16), values, preferred_element_type=jnp.float32
        )

    result = total[...] / jnp.sum(sums[...], axis=1, keepdims=True)
    for k in range(GROUP):
        out_ref[:, k * HD : (k + 1) * HD] = result[k * rows : (k + 1) * rows].astype(jnp.bfloat16)


def attend(where, stacked, starts, kv):
    rows = stacked.shape[0] // GROUP
    vmem = pl.BlockSpec(memory_space=pltpu.VMEM)
    return pl.pallas_call(
        attend_kernel,
        out_shape=jax.ShapeDtypeStruct((rows, GROUP * HD), jnp.bfloat16),
        in_specs=[pl.BlockSpec(memory_space=pltpu.SMEM), vmem, vmem, vmem],
        out_specs=vmem,
        scratch_shapes=[
            pltpu.VMEM((GROUP * rows, HD), jnp.float32),
            pltpu.VMEM((GROUP * rows, HD), jnp.float32),
        ],
        compiler_params=pltpu.CompilerParams(vmem_limit_bytes=24 * 1024 * 1024),
        cost_estimate=pl.CostEstimate(
            flops=4 * GROUP * rows * HD * kv.shape[0] // 2,
            bytes_accessed=kv.size,
            transcendentals=GROUP * rows * kv.shape[0],
        ),
    )(where, stacked, starts, kv)


def over_plane(shard):
    near = from_everyone(shard[None], WIDE).reshape(-1, *shard.shape)
    return from_everyone(near[None], "c").reshape(2, -1, *shard.shape)


def transposed(block):
    n = lax.axis_size("z")
    pairs = [(z * n + h, h * n + z) for z in range(n) for h in range(n)]
    return lax.ppermute(block, ("z", *HEAD), pairs)


def local(tokens, segments, pre_gain, post_gain, w_query, w_key, w_value, w_out):
    rows, width = tokens.shape
    slab = w_key.shape[0]
    ids = jnp.broadcast_to(segments.astype(jnp.bfloat16)[None, :], (16, rows))
    mine = jnp.concatenate(
        [tokens.T, jnp.concatenate([w_key, w_value], axis=1), w_query, ids], axis=0
    )
    turned = transposed(mine)
    whole = lax.all_gather(turned[:width], "z", axis=0, tiled=True)

    turned, tokens, w_out = lax.optimization_barrier((turned, tokens, w_out))
    seg = turned[-1].astype(jnp.float32)
    levels = jnp.arange(DOCS, dtype=jnp.float32)
    counts = jnp.sum((levels[:, None] > seg[None, :]).astype(jnp.float32), axis=1)
    counts = jnp.zeros((16, 2 * HD), jnp.float32).at[0, :DOCS].set(counts).astype(jnp.bfloat16)
    packed = over_plane(jnp.concatenate([turned[width : width + 2 * slab], counts], axis=0))
    weights = packed[:, :, : 2 * slab].reshape(2, -1, 2, slab, 2 * HD).transpose(2, 1, 0, 3, 4)
    weights = weights.reshape(2, D, 2 * HD)
    starts = jnp.sum(packed[:, :, 2 * slab, :DOCS].astype(jnp.float32), axis=(0, 1))

    onehot = (seg[:, None] == levels[None, :]).astype(jnp.float32)
    tok_start = jnp.sum(onehot * starts[None, :], axis=1)
    block = lax.axis_index(("xh", *HEAD))
    index_f = (block * rows + jnp.arange(rows, dtype=jnp.int32)).astype(jnp.float32)
    position = index_f - tok_start
    half = HD // 2
    freq = 10000.0 ** (-(jnp.arange(half, dtype=jnp.float32) / half))
    angle = position[:, None] * freq[None, :]
    cosine, sine = jnp.cos(angle), jnp.sin(angle)
    start_i = tok_start.astype(jnp.int32)
    where = jnp.stack([start_i[0] // rows, block.astype(jnp.int32)])
    starts_col = jnp.tile(start_i, GROUP)[:, None]

    near = lax.axis_size(PLANE)
    few = rows // (near * 2)
    pieces = tokens.reshape(2, near, few, width).transpose(1, 0, 2, 3).reshape(-1, few, width)
    own = lax.all_to_all(pieces, HEAD, 0, 0, tiled=True).transpose(1, 0, 2).reshape(few, D)

    pair = lax.all_gather(w_out.T, "xh", axis=0, tiled=True)
    whole, own, weights, cosine, sine, pair = lax.optimization_barrier(
        (whole, own, weights, cosine, sine, pair)
    )
    out_t = lax.all_gather(pair, "z", axis=0, tiled=True)

    wide = whole.astype(jnp.float32)
    scale = lax.rsqrt(jnp.mean(wide * wide, axis=0, keepdims=True) + EPS)
    normed = (wide * scale * pre_gain[:, None]).astype(jnp.bfloat16)

    def project(columns):
        return lax.dot_general(
            normed, columns, (((0,), (0,)), ((), ())), preferred_element_type=jnp.float32
        )

    kv = project(weights[0])
    rk = rotate(kv[:, :HD], cosine, sine).astype(jnp.bfloat16)
    vb = kv[:, HD:].astype(jnp.bfloat16)
    kv_own, query_weight = lax.optimization_barrier(
        (jnp.concatenate([rk, vb], axis=1), weights[1])
    )
    kv_all = over_plane(kv_own).reshape(-1, 2 * HD)

    query = project(query_weight)
    stacked = jnp.concatenate(
        [
            (rotate(query[:, k * HD : (k + 1) * HD], cosine, sine) * SCALAR ** (-0.5)).astype(
                jnp.bfloat16
            )
            for k in range(GROUP)
        ],
        axis=0,
    )
    out_t = out_t.reshape(-1, 2, slab, 2 * HD).transpose(1, 0, 2, 3).reshape(D, 2 * HD)

    attn = transposed(attend(where, stacked, starts_col, kv_all))
    partial = lax.dot_general(
        attn, out_t, (((1,), (1,)), ((), ())), preferred_element_type=jnp.float32
    ).astype(jnp.bfloat16)

    halves = lax.all_to_all(partial.reshape(2, rows // 2, D), "c", 0, 0, tiled=True)
    halves = (halves[0].astype(jnp.float32) + halves[1].astype(jnp.float32)).astype(jnp.bfloat16)
    blocks = lax.all_to_all(halves.reshape(near, few, D), PLANE, 0, 0, tiled=True)
    proj = jnp.sum(blocks.astype(jnp.float32), axis=0)
    post = lax.rsqrt(jnp.mean(proj * proj, axis=1, keepdims=True) + EPS)
    result = (own.astype(jnp.float32) + proj * post * post_gain[None, :]).astype(jnp.bfloat16)
    result = from_everyone(result, PLANE).reshape(rows // 2, D)
    return from_everyone(result, "c").reshape(rows, D)


def solution(mesh):
    finer = Mesh(mesh.devices.reshape(2, 16, 2, 4, 2), ("xh", "z", "xl", "y", "c"))
    in_specs = (
        P(SEQ, HEAD),
        P(SEQ),
        P(),
        P(),
        P(SEQ, HEAD),
        P(SEQ, HEAD),
        P(SEQ, HEAD),
        P(HEAD, SEQ),
    )
    return jax.shard_map(
        local, mesh=finer, in_specs=in_specs, out_specs=P(SEQ, None), check_vma=False
    )
```

```python
import jax
import jax.numpy as jnp
from jax import lax
from jax.experimental import pallas as pl
from jax.experimental.pallas import tpu as pltpu
from jax.sharding import Mesh
from jax.sharding import PartitionSpec as P

D = 4608
HD = 128
GROUP = 2
SCALAR = 144
DOCS = 8
SEQ = ("xh", "z")
HEAD = ("xl", "y", "c")
PLANE = ("xl", "y")

EPS = 1e-06
CAP = 50.0


def from_everyone(shard, axis):
    copies = jnp.broadcast_to(shard, (lax.axis_size(axis), *shard.shape))
    return lax.all_to_all(copies, axis, split_axis=0, concat_axis=0, tiled=True)


def rotate(values, cosine, sine):
    half = values.shape[1] // 2
    first = values[:, :half]
    second = values[:, half:]
    return jnp.concatenate(
        [first * cosine - second * sine, second * cosine + first * sine], axis=1
    )


def attend_kernel(where_ref, query_ref, start_ref, kv_hbm, out_ref, held, sums, total, sem):
    rows = query_ref.shape[0] // GROUP
    low = where_ref[0]
    own = where_ref[1]
    halves = where_ref[2]

    def fetch(j):
        place = (lax.rem(j, halves) * 2 + lax.div(j, halves)) * rows
        return pltpu.make_async_copy(
            kv_hbm.at[pl.ds(pl.multiple_of(place, rows), rows), :], held.at[j], sem.at[j]
        )

    @pl.loop(low, own + 1)
    def _(j):
        fetch(j).start()

    sums[...] = jnp.zeros_like(sums)
    total[...] = jnp.zeros_like(total)
    shape = (GROUP * rows, rows)
    row = lax.broadcasted_iota(jnp.int32, shape, 0)
    index = own * rows + jnp.where(row >= rows, row - rows, row)
    column = lax.broadcasted_iota(jnp.int32, shape, 1)

    @pl.loop(low, own + 1)
    def _(j):
        fetch(j).wait()
        keys = held[j, :, :HD]
        values = held[j, :, HD:]
        scores = lax.dot_general(
            query_ref[...], keys, (((1,), (1,)), ((), ())), preferred_element_type=jnp.float32
        )
        weights = jnp.exp(CAP * jnp.tanh(scores * (1.0 / CAP)))
        key_index = j * rows + column
        allowed = (key_index >= start_ref[...]) & (key_index <= index)
        weights = jnp.where(allowed, weights, 0.0)
        part = weights[:, :HD]
        for k in range(1, rows // HD):
            part = part + weights[:, k * HD : (k + 1) * HD]
        sums[...] += part
        total[...] += jnp.dot(
            weights.astype(jnp.bfloat16), values, preferred_element_type=jnp.float32
        )

    result = total[...] / jnp.sum(sums[...], axis=1, keepdims=True)
    for k in range(GROUP):
        out_ref[:, k * HD : (k + 1) * HD] = result[k * rows : (k + 1) * rows].astype(jnp.bfloat16)


def attend(where, stacked, starts, kv):
    rows = stacked.shape[0] // GROUP
    blocks = kv.shape[0] // rows
    vmem = pl.BlockSpec(memory_space=pltpu.VMEM)
    return pl.pallas_call(
        attend_kernel,
        out_shape=jax.ShapeDtypeStruct((rows, GROUP * HD), jnp.bfloat16),
        in_specs=[
            pl.BlockSpec(memory_space=pltpu.SMEM),
            vmem,
            vmem,
            pl.BlockSpec(memory_space=pl.ANY),
        ],
        out_specs=vmem,
        scratch_shapes=[
            pltpu.VMEM((blocks, rows, 2 * HD), jnp.bfloat16),
            pltpu.VMEM((GROUP * rows, HD), jnp.float32),
            pltpu.VMEM((GROUP * rows, HD), jnp.float32),
            pltpu.SemaphoreType.DMA((blocks,)),
        ],
        compiler_params=pltpu.CompilerParams(vmem_limit_bytes=60 * 1024 * 1024),
        cost_estimate=pl.CostEstimate(
            flops=4 * GROUP * rows * HD * kv.shape[0] // 2,
            bytes_accessed=kv.size,
            transcendentals=GROUP * rows * kv.shape[0],
        ),
    )(where, stacked, starts, kv)


def local(tokens, segments, pre_gain, post_gain, w_query, w_key, w_value, w_out):
    rows, width = tokens.shape
    deep = lax.axis_size("z")
    mine = jnp.concatenate([w_key, w_value, w_query, w_out.T], axis=1)
    weights = lax.all_gather(mine, "z", axis=0, tiled=True)
    deep_half = weights.shape[0]

    ids = jnp.broadcast_to(segments.astype(jnp.bfloat16)[None, :], (16, rows))
    slices = jnp.concatenate([tokens.T, ids], axis=0)
    slices = lax.ppermute(slices, ("xh", "xl"), [(0, 0), (1, 2), (2, 1), (3, 3)])
    slices = from_everyone(slices[None], PLANE).reshape(-1, *slices.shape)
    slices = from_everyone(slices[None], "c").reshape(2, 2, -1, *slices.shape[1:])
    seg = slices[0, :, 0, width].astype(jnp.float32)
    levels = jnp.arange(DOCS, dtype=jnp.float32)
    counts = jnp.sum((levels[:, None, None] > seg[None]).astype(jnp.float32), axis=(1, 2))
    starts = jnp.sum(from_everyone(counts[None], "z").reshape(-1, DOCS), axis=0)
    onehot = (seg[:, :, None] == levels).astype(jnp.float32)
    tok_start = jnp.sum(onehot * starts, axis=2)
    side = lax.axis_index("xh")
    place = lax.axis_index("z")
    blocks = (jnp.arange(2, dtype=jnp.int32) * deep + place)[:, None] * rows
    index_f = (blocks + jnp.arange(rows, dtype=jnp.int32)).astype(jnp.float32)
    position = (index_f - tok_start).reshape(2 * rows)
    half = HD // 2
    freq = 10000.0 ** (-(jnp.arange(half, dtype=jnp.float32) / half))
    angle = position[:, None] * freq[None, :]
    cosine, sine = jnp.cos(angle), jnp.sin(angle)
    start_i = lax.dynamic_index_in_dim(tok_start, side, 0, keepdims=False).astype(jnp.int32)
    where = jnp.stack(
        [start_i[0] // rows, (side * deep + place).astype(jnp.int32), jnp.int32(deep)]
    )
    starts_col = jnp.tile(start_i, GROUP)[:, None]

    wide = slices[:, :, :, :width].transpose(1, 2, 0, 3, 4).reshape(2, deep_half, rows)
    wide = wide.astype(jnp.float32)
    squares = jnp.sum(lax.all_gather(jnp.sum(wide * wide, axis=1), "xh", axis=0), axis=0)
    scale = lax.rsqrt(squares / D + EPS)
    gain = lax.dynamic_slice_in_dim(pre_gain, side * deep_half, deep_half, 0)
    normed = (wide * scale[:, None, :] * gain[None, :, None]).astype(jnp.bfloat16)
    normed = normed.transpose(0, 2, 1).reshape(2 * rows, deep_half)
    normed, cosine, sine, weights = lax.optimization_barrier((normed, cosine, sine, weights))

    def project(columns):
        part = jnp.dot(normed, columns, preferred_element_type=jnp.float32).astype(jnp.bfloat16)
        both = lax.all_gather(part, "xh", axis=0)
        return both[0].astype(jnp.float32) + both[1].astype(jnp.float32)

    kv = project(weights[:, : 2 * HD])
    rk = rotate(kv[:, :HD], cosine, sine).astype(jnp.bfloat16)
    vb = kv[:, HD:].astype(jnp.bfloat16)
    kv_pair, query_weight, out_weight, tokens = lax.optimization_barrier(
        (
            jnp.concatenate([rk, vb], axis=1),
            weights[:, 2 * HD : 4 * HD],
            weights[:, 4 * HD :],
            tokens,
        )
    )
    kv_all = lax.all_gather(kv_pair, "z", axis=0, tiled=True)

    query = lax.dynamic_slice_in_dim(project(query_weight), side * rows, rows, 0)
    own_cos = lax.dynamic_slice_in_dim(cosine, side * rows, rows, 0)
    own_sin = lax.dynamic_slice_in_dim(sine, side * rows, rows, 0)
    stacked = jnp.concatenate(
        [
            (rotate(query[:, k * HD : (k + 1) * HD], own_cos, own_sin) * SCALAR ** (-0.5)).astype(
                jnp.bfloat16
            )
            for k in range(GROUP)
        ],
        axis=0,
    )
    out_t = from_everyone(out_weight[None], "xh").reshape(D, GROUP * HD)
    near = lax.axis_size(PLANE)
    few = rows // (near * 2)
    pieces = tokens.reshape(2, near, few, width).transpose(1, 0, 2, 3).reshape(-1, few, width)
    own = lax.all_to_all(pieces, HEAD, 0, 0, tiled=True).transpose(1, 0, 2).reshape(few, D)
    kv_all, stacked, out_t, own = lax.optimization_barrier((kv_all, stacked, out_t, own))

    attn = attend(where, stacked, starts_col, kv_all)
    partial = lax.dot_general(
        attn, out_t, (((1,), (1,)), ((), ())), preferred_element_type=jnp.float32
    ).astype(jnp.bfloat16)

    halves = lax.all_to_all(partial.reshape(2, rows // 2, D), "c", 0, 0, tiled=True)
    halves = (halves[0].astype(jnp.float32) + halves[1].astype(jnp.float32)).astype(jnp.bfloat16)
    pieces = lax.all_to_all(halves.reshape(near, few, D), PLANE, 0, 0, tiled=True)
    proj = jnp.sum(pieces.astype(jnp.float32), axis=0)
    post = lax.rsqrt(jnp.mean(proj * proj, axis=1, keepdims=True) + EPS)
    result = (own.astype(jnp.float32) + proj * post * post_gain[None, :]).astype(jnp.bfloat16)
    result = from_everyone(result, PLANE).reshape(rows // 2, D)
    return from_everyone(result, "c").reshape(rows, D)


def solution(mesh):
    finer = Mesh(mesh.devices.reshape(2, 16, 2, 4, 2), ("xh", "z", "xl", "y", "c"))
    in_specs = (
        P(SEQ, HEAD),
        P(SEQ),
        P(),
        P(),
        P(SEQ, HEAD),
        P(SEQ, HEAD),
        P(SEQ, HEAD),
        P(HEAD, SEQ),
    )
    return jax.shard_map(
        local, mesh=finer, in_specs=in_specs, out_specs=P(SEQ, None), check_vma=False
    )
```

```python
import jax
import jax.numpy as jnp
from jax import lax
from jax.experimental import pallas as pl
from jax.experimental.pallas import tpu as pltpu
from jax.sharding import Mesh
from jax.sharding import PartitionSpec as P

D = 4608
HD = 128
GROUP = 2
SCALAR = 144
DOCS = 8
SEQ = ("xh", "z")
HEAD = ("xl", "y", "c")
PLANE = ("xl", "y")

EPS = 1e-06
CAP = 50.0


def from_everyone(shard, axis):
    copies = jnp.broadcast_to(shard, (lax.axis_size(axis), *shard.shape))
    return lax.all_to_all(copies, axis, split_axis=0, concat_axis=0, tiled=True)


def rotate(values, cosine, sine):
    half = values.shape[1] // 2
    first = values[:, :half]
    second = values[:, half:]
    return jnp.concatenate(
        [first * cosine - second * sine, second * cosine + first * sine], axis=1
    )


def attend_kernel(
    where_ref, query_ref, start_ref, kv_hbm, near_ref, away_ref, held, sums, total, sem
):
    rows = query_ref.shape[0] // GROUP
    low = where_ref[0]
    own = where_ref[1]
    halves = where_ref[2]

    def fetch(j):
        place = (lax.rem(j, halves) * 2 + lax.div(j, halves)) * rows
        return pltpu.make_async_copy(
            kv_hbm.at[pl.ds(pl.multiple_of(place, rows), rows), :], held.at[j], sem.at[j]
        )

    @pl.loop(low, own + 1)
    def _(j):
        fetch(j).start()

    sums[...] = jnp.zeros_like(sums)
    total[...] = jnp.zeros_like(total)

    def gather(j, count, masked):
        for k in range(count):
            fetch(j + k).wait()
        keys = held[pl.ds(j, count), :, :HD].reshape(count * rows, HD)
        values = held[pl.ds(j, count), :, HD:].reshape(count * rows, HD)
        scores = lax.dot_general(
            query_ref[...], keys, (((1,), (1,)), ((), ())), preferred_element_type=jnp.float32
        )
        weights = jnp.exp(CAP * jnp.tanh(scores * (1.0 / CAP)))
        if masked:
            shape = (GROUP * rows, rows)
            row = lax.broadcasted_iota(jnp.int32, shape, 0)
            index = own * rows + jnp.where(row >= rows, row - rows, row)
            key_index = j * rows + lax.broadcasted_iota(jnp.int32, shape, 1)
            allowed = (key_index >= start_ref[...]) & (key_index <= index)
            weights = jnp.where(allowed, weights, 0.0)
        part = weights[:, :HD]
        for k in range(1, count * rows // HD):
            part = part + weights[:, k * HD : (k + 1) * HD]
        sums[...] += part
        total[...] += jnp.dot(
            weights.astype(jnp.bfloat16), values, preferred_element_type=jnp.float32
        )

    done = low + 1
    for count in (4, 2, 1):
        steps = lax.div(jnp.maximum(own - done, 0), count)

        @pl.loop(0, steps)
        def _(i, done=done, count=count):
            gather(done + i * count, count, False)

        done = done + steps * count

    seen = start_ref[...] < own * rows
    sums[...] = jnp.where(seen, sums[...], 0.0)
    total[...] = jnp.where(seen, total[...], 0.0)

    @pl.when(low < own)
    def _():
        gather(low, 1, True)

    gather(own, 1, True)

    result = total[...] / jnp.sum(sums[...], axis=1, keepdims=True)
    south = where_ref[3] == 0
    for k in range(GROUP):
        upper = result[k * rows : k * rows + rows // 2]
        lower = result[k * rows + rows // 2 : (k + 1) * rows]
        columns = slice(k * HD, (k + 1) * HD)
        near_ref[:, columns] = jnp.where(south, upper, lower).astype(jnp.bfloat16)
        away_ref[:, columns] = jnp.where(south, lower, upper).astype(jnp.bfloat16)


def attend(where, stacked, starts, kv):
    rows = stacked.shape[0] // GROUP
    blocks = kv.shape[0] // rows
    vmem = pl.BlockSpec(memory_space=pltpu.VMEM)
    return pl.pallas_call(
        attend_kernel,
        out_shape=[jax.ShapeDtypeStruct((rows // 2, GROUP * HD), jnp.bfloat16)] * 2,
        in_specs=[
            pl.BlockSpec(memory_space=pltpu.SMEM),
            vmem,
            vmem,
            pl.BlockSpec(memory_space=pltpu.HBM),
        ],
        out_specs=[vmem, vmem],
        scratch_shapes=[
            pltpu.VMEM((blocks, rows, 2 * HD), jnp.bfloat16),
            pltpu.VMEM((GROUP * rows, HD), jnp.float32),
            pltpu.VMEM((GROUP * rows, HD), jnp.float32),
            pltpu.SemaphoreType.DMA((blocks,)),
        ],
        compiler_params=pltpu.CompilerParams(vmem_limit_bytes=54 * 1024 * 1024),
        cost_estimate=pl.CostEstimate(
            flops=4 * GROUP * rows * HD * kv.shape[0] // 2,
            bytes_accessed=kv.size,
            transcendentals=GROUP * rows * kv.shape[0],
        ),
    )(where, stacked, starts, kv)


def finish_kernel(side_ref, part_ref, both_ref, cos_ref, sin_ref, out_ref):
    other = jnp.where(side_ref[0] == 0, both_ref[1], both_ref[0])
    keys = part_ref[:, :HD] + other[:, :HD].astype(jnp.float32)
    turned = keys * cos_ref[...] + pltpu.roll(keys, HD // 2, 1) * sin_ref[...]
    out_ref[:, :HD] = turned.astype(jnp.bfloat16)
    values = part_ref[:, HD:] + other[:, HD:].astype(jnp.float32)
    out_ref[:, HD:] = values.astype(jnp.bfloat16)


def finish(side, part, both, cosine, sine):
    vmem = pl.BlockSpec(memory_space=pltpu.VMEM)
    return pl.pallas_call(
        finish_kernel,
        out_shape=jax.ShapeDtypeStruct(part.shape, jnp.bfloat16),
        in_specs=[pl.BlockSpec(memory_space=pltpu.SMEM), vmem, vmem, vmem, vmem],
        out_specs=vmem,
        compiler_params=pltpu.CompilerParams(vmem_limit_bytes=16 * 1024 * 1024),
    )(side, part, both, cosine, sine)


def local(tokens, segments, pre_gain, post_gain, w_query, w_key, w_value, w_out):
    rows, width = tokens.shape
    deep = lax.axis_size("z")
    mine = jnp.concatenate([w_key, w_value, w_query, w_out.T], axis=1)
    weights = lax.all_gather(mine, "z", axis=0, tiled=True)
    deep_half = weights.shape[0]

    ids = jnp.broadcast_to(segments.astype(jnp.bfloat16)[None, :], (16, rows))
    slices = jnp.concatenate([tokens.T, ids], axis=0)
    slices = lax.ppermute(slices, ("xh", "xl"), [(0, 0), (1, 2), (2, 1), (3, 3)])
    slices = from_everyone(slices[None], PLANE).reshape(-1, *slices.shape)
    slices = from_everyone(slices[None], "c").reshape(2, 2, -1, *slices.shape[1:])
    seg = slices[0, :, 0, width].astype(jnp.float32)
    levels = jnp.arange(DOCS, dtype=jnp.float32)
    counts = jnp.sum((levels[:, None, None] > seg[None]).astype(jnp.float32), axis=(1, 2))
    starts = jnp.sum(from_everyone(counts[None], "z").reshape(-1, DOCS), axis=0)
    onehot = (seg[:, :, None] == levels).astype(jnp.float32)
    tok_start = jnp.sum(onehot * starts, axis=2)
    side = lax.axis_index("xh")
    place = lax.axis_index("z")
    blocks = (jnp.arange(2, dtype=jnp.int32) * deep + place)[:, None] * rows
    index_f = (blocks + jnp.arange(rows, dtype=jnp.int32)).astype(jnp.float32)
    position = (index_f - tok_start).reshape(2 * rows)
    half = HD // 2
    freq = 10000.0 ** (-(jnp.arange(half, dtype=jnp.float32) / half))
    angle = position[:, None] * freq[None, :]
    cosine, sine = jnp.cos(angle), jnp.sin(angle)
    start_i = lax.dynamic_index_in_dim(tok_start, side, 0, keepdims=False).astype(jnp.int32)
    where = jnp.stack(
        [
            start_i[0] // rows,
            (side * deep + place).astype(jnp.int32),
            jnp.int32(deep),
            lax.axis_index("c").astype(jnp.int32),
        ]
    )
    starts_col = jnp.tile(start_i, GROUP)[:, None]

    wide = slices[:, :, :, :width].transpose(1, 2, 0, 3, 4).reshape(2, deep_half, rows)
    wide = wide.astype(jnp.float32)
    squares = jnp.sum(lax.all_gather(jnp.sum(wide * wide, axis=1), "xh", axis=0), axis=0)
    scale = lax.rsqrt(squares / D + EPS)
    gain = lax.dynamic_slice_in_dim(pre_gain, side * deep_half, deep_half, 0)
    normed = (wide * scale[:, None, :] * gain[None, :, None]).astype(jnp.bfloat16)
    normed = normed.transpose(0, 2, 1).reshape(2 * rows, deep_half)
    near = lax.axis_size(PLANE)
    few = rows // (near * 2)
    pieces = tokens.reshape(2, near, few, width).transpose(1, 0, 2, 3).reshape(-1, few, width)
    own = lax.all_to_all(pieces, HEAD, 0, 0, tiled=True).transpose(1, 0, 2).reshape(few, D)
    cos_wide = jnp.concatenate([cosine, cosine], axis=1)
    sin_wide = jnp.concatenate([-sine, sine], axis=1)
    normed, cosine, sine, cos_wide, sin_wide, weights, own = lax.optimization_barrier(
        (normed, cosine, sine, cos_wide, sin_wide, weights, own)
    )

    def project(columns):
        return jnp.dot(normed, columns, preferred_element_type=jnp.float32)

    part = project(weights[:, : 2 * HD])
    both = lax.all_gather(part.astype(jnp.bfloat16), "xh", axis=0)
    kv_pair = finish(side.astype(jnp.int32)[None], part, both, cos_wide, sin_wide)
    kv_pair, weights = lax.optimization_barrier((kv_pair, weights))
    kv_all = lax.all_gather(kv_pair, "z", axis=0, tiled=True)

    query = project(weights[:, 2 * HD : 4 * HD]).reshape(2, rows, 2 * HD)
    query = jnp.sum(lax.all_to_all(query, "xh", 0, 0, tiled=True), axis=0)
    own_cos = lax.dynamic_slice_in_dim(cosine, side * rows, rows, 0)
    own_sin = lax.dynamic_slice_in_dim(sine, side * rows, rows, 0)
    stacked = jnp.concatenate(
        [
            (rotate(query[:, k * HD : (k + 1) * HD], own_cos, own_sin) * SCALAR ** (-0.5)).astype(
                jnp.bfloat16
            )
            for k in range(GROUP)
        ],
        axis=0,
    )
    out_t = from_everyone(weights[None, :, 4 * HD :], "xh").reshape(D, GROUP * HD)
    swap = [(0, 1), (1, 0)]
    out_far = lax.ppermute(out_t, "c", swap)
    kv_all, stacked, out_t, out_far = lax.optimization_barrier((kv_all, stacked, out_t, out_far))

    kept, away = attend(where, stacked, starts_col, kv_all)
    far = lax.ppermute(away, "c", swap)

    def through(part, rows_of):
        return lax.dot_general(
            part, rows_of, (((1,), (1,)), ((), ())), preferred_element_type=jnp.float32
        )

    near_part = through(kept, out_t)
    near_part, far = lax.optimization_barrier((near_part, far))
    halves = (near_part + through(far, out_far)).astype(jnp.bfloat16)
    pieces = lax.all_to_all(halves.reshape(near, few, D), PLANE, 0, 0, tiled=True)
    proj = jnp.sum(pieces.astype(jnp.float32), axis=0)
    post = lax.rsqrt(jnp.mean(proj * proj, axis=1, keepdims=True) + EPS)
    result = (own.astype(jnp.float32) + proj * post * post_gain[None, :]).astype(jnp.bfloat16)
    result = from_everyone(result, PLANE).reshape(rows // 2, D)
    other = lax.ppermute(result, "c", swap)
    mine_first = (jnp.arange(2) == lax.axis_index("c"))[:, None, None]
    return jnp.where(mine_first, result[None], other[None]).reshape(rows, D)


def solution(mesh):
    finer = Mesh(mesh.devices.reshape(2, 16, 2, 4, 2), ("xh", "z", "xl", "y", "c"))
    in_specs = (
        P(SEQ, HEAD),
        P(SEQ),
        P(),
        P(),
        P(SEQ, HEAD),
        P(SEQ, HEAD),
        P(SEQ, HEAD),
        P(HEAD, SEQ),
    )
    return jax.shard_map(
        local, mesh=finer, in_specs=in_specs, out_specs=P(SEQ, None), check_vma=False
    )
```

```python
import jax
import jax.numpy as jnp
from jax import lax
from jax.experimental import pallas as pl
from jax.experimental.pallas import tpu as pltpu
from jax.sharding import Mesh
from jax.sharding import PartitionSpec as P

D = 4608
HD = 128
GROUP = 2
SCALAR = 144
DOCS = 8
SEQ = ("xh", "z")
HEAD = ("xl", "y", "c")
PLANE = ("xl", "y")

EPS = 1e-06
CAP = 50.0


def from_everyone(shard, axis):
    copies = jnp.broadcast_to(shard, (lax.axis_size(axis), *shard.shape))
    return lax.all_to_all(copies, axis, split_axis=0, concat_axis=0, tiled=True)


def rotate(values, cosine, sine):
    half = values.shape[1] // 2
    first = values[:, :half]
    second = values[:, half:]
    return jnp.concatenate(
        [first * cosine - second * sine, second * cosine + first * sine], axis=1
    )


def attend_kernel(
    where_ref, query_ref, start_ref, kv_hbm, near_ref, away_ref, held, sums, total, sem
):
    rows = query_ref.shape[0] // GROUP
    low = where_ref[0]
    own = where_ref[1]
    halves = where_ref[2]

    def fetch(j):
        place = (lax.rem(j, halves) * 2 + lax.div(j, halves)) * rows
        return pltpu.make_async_copy(
            kv_hbm.at[pl.ds(pl.multiple_of(place, rows), rows), :], held.at[j], sem.at[j]
        )

    @pl.loop(low, own + 1)
    def _(j):
        fetch(j).start()

    sums[...] = jnp.zeros_like(sums)
    total[...] = jnp.zeros_like(total)

    def gather(j, count, masked):
        for k in range(count):
            fetch(j + k).wait()
        keys = held[pl.ds(j, count), :, :HD].reshape(count * rows, HD)
        values = held[pl.ds(j, count), :, HD:].reshape(count * rows, HD)
        scores = lax.dot_general(
            query_ref[...], keys, (((1,), (1,)), ((), ())), preferred_element_type=jnp.float32
        )
        weights = jnp.exp(CAP * jnp.tanh(scores * (1.0 / CAP)))
        if masked:
            shape = (GROUP * rows, rows)
            row = lax.broadcasted_iota(jnp.int32, shape, 0)
            index = own * rows + jnp.where(row >= rows, row - rows, row)
            key_index = j * rows + lax.broadcasted_iota(jnp.int32, shape, 1)
            allowed = (key_index >= start_ref[...]) & (key_index <= index)
            weights = jnp.where(allowed, weights, 0.0)
        part = weights[:, :HD]
        for k in range(1, count * rows // HD):
            part = part + weights[:, k * HD : (k + 1) * HD]
        sums[...] += part
        total[...] += jnp.dot(
            weights.astype(jnp.bfloat16), values, preferred_element_type=jnp.float32
        )

    done = low + 1
    for count in (4, 2, 1):
        steps = lax.div(jnp.maximum(own - done, 0), count)

        @pl.loop(0, steps)
        def _(i, done=done, count=count):
            gather(done + i * count, count, False)

        done = done + steps * count

    seen = start_ref[...] < own * rows
    sums[...] = jnp.where(seen, sums[...], 0.0)
    total[...] = jnp.where(seen, total[...], 0.0)

    @pl.when(low < own)
    def _():
        gather(low, 1, True)

    gather(own, 1, True)

    result = total[...] / jnp.sum(sums[...], axis=1, keepdims=True)
    south = where_ref[3] == 0
    for k in range(GROUP):
        upper = result[k * rows : k * rows + rows // 2]
        lower = result[k * rows + rows // 2 : (k + 1) * rows]
        columns = slice(k * HD, (k + 1) * HD)
        near_ref[:, columns] = jnp.where(south, upper, lower).astype(jnp.bfloat16)
        away_ref[:, columns] = jnp.where(south, lower, upper).astype(jnp.bfloat16)


def attend(where, stacked, starts, kv):
    rows = stacked.shape[0] // GROUP
    blocks = kv.shape[0] // rows
    vmem = pl.BlockSpec(memory_space=pltpu.VMEM)
    return pl.pallas_call(
        attend_kernel,
        out_shape=[jax.ShapeDtypeStruct((rows // 2, GROUP * HD), jnp.bfloat16)] * 2,
        in_specs=[
            pl.BlockSpec(memory_space=pltpu.SMEM),
            vmem,
            vmem,
            pl.BlockSpec(memory_space=pltpu.HBM),
        ],
        out_specs=[vmem, vmem],
        scratch_shapes=[
            pltpu.VMEM((blocks, rows, 2 * HD), jnp.bfloat16),
            pltpu.VMEM((GROUP * rows, HD), jnp.float32),
            pltpu.VMEM((GROUP * rows, HD), jnp.float32),
            pltpu.SemaphoreType.DMA((blocks,)),
        ],
        compiler_params=pltpu.CompilerParams(vmem_limit_bytes=54 * 1024 * 1024),
        cost_estimate=pl.CostEstimate(
            flops=4 * GROUP * rows * HD * kv.shape[0] // 2,
            bytes_accessed=kv.size,
            transcendentals=GROUP * rows * kv.shape[0],
        ),
    )(where, stacked, starts, kv)


def finish_kernel(side_ref, part_ref, both_ref, cos_ref, sin_ref, out_ref):
    other = jnp.where(side_ref[0] == 0, both_ref[1], both_ref[0])
    keys = part_ref[:, :HD] + other[:, :HD].astype(jnp.float32)
    turned = keys * cos_ref[...] + pltpu.roll(keys, HD // 2, 1) * sin_ref[...]
    out_ref[:, :HD] = turned.astype(jnp.bfloat16)
    values = part_ref[:, HD:] + other[:, HD:].astype(jnp.float32)
    out_ref[:, HD:] = values.astype(jnp.bfloat16)


def finish(side, part, both, cosine, sine):
    vmem = pl.BlockSpec(memory_space=pltpu.VMEM)
    return pl.pallas_call(
        finish_kernel,
        out_shape=jax.ShapeDtypeStruct(part.shape, jnp.bfloat16),
        in_specs=[pl.BlockSpec(memory_space=pltpu.SMEM), vmem, vmem, vmem, vmem],
        out_specs=vmem,
        compiler_params=pltpu.CompilerParams(vmem_limit_bytes=16 * 1024 * 1024),
    )(side, part, both, cosine, sine)


def local(tokens, segments, pre_gain, post_gain, w_query, w_key, w_value, w_out):
    rows, width = tokens.shape
    deep = lax.axis_size("z")
    mine = jnp.concatenate([w_key, w_value, w_query, w_out.T], axis=1)
    weights = lax.all_gather(mine, "z", axis=0, tiled=True)
    deep_half = weights.shape[0]

    ids = jnp.broadcast_to(segments.astype(jnp.bfloat16)[None, :], (16, rows))
    slices = jnp.concatenate([tokens.T, ids], axis=0)
    slices = lax.ppermute(slices, ("xh", "xl"), [(0, 0), (1, 2), (2, 1), (3, 3)])
    slices = from_everyone(slices[None], PLANE).reshape(-1, *slices.shape)
    slices = from_everyone(slices[None], "c").reshape(2, 2, -1, *slices.shape[1:])
    seg = slices[0, :, 0, width].astype(jnp.float32)
    levels = jnp.arange(DOCS, dtype=jnp.float32)
    counts = jnp.sum((levels[:, None, None] > seg[None]).astype(jnp.float32), axis=(1, 2))
    starts = jnp.sum(from_everyone(counts[None], "z").reshape(-1, DOCS), axis=0)
    onehot = (seg[:, :, None] == levels).astype(jnp.float32)
    tok_start = jnp.sum(onehot * starts, axis=2)
    side = lax.axis_index("xh")
    place = lax.axis_index("z")
    blocks = (jnp.arange(2, dtype=jnp.int32) * deep + place)[:, None] * rows
    index_f = (blocks + jnp.arange(rows, dtype=jnp.int32)).astype(jnp.float32)
    position = (index_f - tok_start).reshape(2 * rows)
    half = HD // 2
    freq = 10000.0 ** (-(jnp.arange(half, dtype=jnp.float32) / half))
    angle = position[:, None] * freq[None, :]
    cosine, sine = jnp.cos(angle), jnp.sin(angle)
    start_i = lax.dynamic_index_in_dim(tok_start, side, 0, keepdims=False).astype(jnp.int32)
    where = jnp.stack(
        [
            start_i[0] // rows,
            (side * deep + place).astype(jnp.int32),
            jnp.int32(deep),
            lax.axis_index("c").astype(jnp.int32),
        ]
    )
    starts_col = jnp.tile(start_i, GROUP)[:, None]

    wide = slices[:, :, :, :width].transpose(1, 2, 0, 3, 4).reshape(2, deep_half, rows)
    wide = wide.astype(jnp.float32)
    squares = jnp.sum(lax.all_gather(jnp.sum(wide * wide, axis=1), "xh", axis=0), axis=0)
    scale = lax.rsqrt(squares / D + EPS)
    gain = lax.dynamic_slice_in_dim(pre_gain, side * deep_half, deep_half, 0)
    normed = (wide * scale[:, None, :] * gain[None, :, None]).astype(jnp.bfloat16)
    normed = normed.transpose(0, 2, 1).reshape(2 * rows, deep_half)
    cos_wide = jnp.concatenate([cosine, cosine], axis=1)
    sin_wide = jnp.concatenate([-sine, sine], axis=1)
    normed, cosine, sine, cos_wide, sin_wide, weights = lax.optimization_barrier(
        (normed, cosine, sine, cos_wide, sin_wide, weights)
    )

    def project(columns):
        return jnp.dot(normed, columns, preferred_element_type=jnp.float32)

    part = project(weights[:, : 2 * HD])
    both = lax.all_gather(part.astype(jnp.bfloat16), "xh", axis=0)
    kv_pair = finish(side.astype(jnp.int32)[None], part, both, cos_wide, sin_wide)
    kv_pair, weights, tokens = lax.optimization_barrier((kv_pair, weights, tokens))
    kv_all = lax.all_gather(kv_pair, "z", axis=0, tiled=True)

    query = project(weights[:, 2 * HD : 4 * HD]).reshape(2, rows, 2 * HD)
    query = jnp.sum(lax.all_to_all(query, "xh", 0, 0, tiled=True), axis=0)
    own_cos = lax.dynamic_slice_in_dim(cosine, side * rows, rows, 0)
    own_sin = lax.dynamic_slice_in_dim(sine, side * rows, rows, 0)
    stacked = jnp.concatenate(
        [
            (rotate(query[:, k * HD : (k + 1) * HD], own_cos, own_sin) * SCALAR ** (-0.5)).astype(
                jnp.bfloat16
            )
            for k in range(GROUP)
        ],
        axis=0,
    )
    out_t = from_everyone(weights[None, :, 4 * HD :], "xh").reshape(D, GROUP * HD)
    near = lax.axis_size(PLANE)
    few = rows // (near * 2)
    pieces = tokens.reshape(2, near, few, width).transpose(1, 0, 2, 3).reshape(-1, few, width)
    own = lax.all_to_all(pieces, HEAD, 0, 0, tiled=True).transpose(1, 0, 2).reshape(few, D)
    swap = [(0, 1), (1, 0)]
    out_far = lax.ppermute(out_t, "c", swap)
    kv_all, stacked, out_t, out_far, own = lax.optimization_barrier(
        (kv_all, stacked, out_t, out_far, own)
    )

    kept, away = attend(where, stacked, starts_col, kv_all)
    far = lax.ppermute(away, "c", swap)

    def through(part, rows_of):
        return lax.dot_general(
            part, rows_of, (((1,), (1,)), ((), ())), preferred_element_type=jnp.float32
        )

    near_part = through(kept, out_t)
    near_part, far = lax.optimization_barrier((near_part, far))
    halves = (near_part + through(far, out_far)).astype(jnp.bfloat16)
    pieces = lax.all_to_all(halves.reshape(near, few, D), PLANE, 0, 0, tiled=True)
    proj = jnp.sum(pieces.astype(jnp.float32), axis=0)
    post = lax.rsqrt(jnp.mean(proj * proj, axis=1, keepdims=True) + EPS)
    result = (own.astype(jnp.float32) + proj * post * post_gain[None, :]).astype(jnp.bfloat16)
    result = from_everyone(result, PLANE).reshape(rows // 2, D)
    other = lax.ppermute(result, "c", swap)
    mine_first = (jnp.arange(2) == lax.axis_index("c"))[:, None, None]
    return jnp.where(mine_first, result[None], other[None]).reshape(rows, D)


def solution(mesh):
    finer = Mesh(mesh.devices.reshape(2, 16, 2, 4, 2), ("xh", "z", "xl", "y", "c"))
    in_specs = (
        P(SEQ, HEAD),
        P(SEQ),
        P(),
        P(),
        P(SEQ, HEAD),
        P(SEQ, HEAD),
        P(SEQ, HEAD),
        P(HEAD, SEQ),
    )
    return jax.shard_map(
        local, mesh=finer, in_specs=in_specs, out_specs=P(SEQ, None), check_vma=False
    )
```

```python
import jax
import jax.numpy as jnp
from jax import lax
from jax.experimental import pallas as pl
from jax.experimental.pallas import tpu as pltpu
from jax.sharding import Mesh
from jax.sharding import PartitionSpec as P

D = 4608
HD = 128
GROUP = 2
SCALAR = 144
DOCS = 8
SEQ = ("xh", "z")
HEAD = ("xl", "y", "c")
PLANE = ("xl", "y")

EPS = 1e-06
CAP = 50.0


def from_everyone(shard, axis):
    copies = jnp.broadcast_to(shard, (lax.axis_size(axis), *shard.shape))
    return lax.all_to_all(copies, axis, split_axis=0, concat_axis=0, tiled=True)


def rotate(values, cosine, sine):
    half = values.shape[1] // 2
    first = values[:, :half]
    second = values[:, half:]
    return jnp.concatenate(
        [first * cosine - second * sine, second * cosine + first * sine], axis=1
    )


def attend_kernel(
    where_ref, query_ref, start_ref, kv_hbm, near_ref, away_ref, held, sums, total, sem
):
    rows = query_ref.shape[0] // GROUP
    low = where_ref[0]
    own = where_ref[1]
    halves = where_ref[2]

    def fetch(j):
        place = (lax.rem(j, halves) * 2 + lax.div(j, halves)) * rows
        return pltpu.make_async_copy(
            kv_hbm.at[pl.ds(pl.multiple_of(place, rows), rows), :], held.at[j], sem.at[j]
        )

    @pl.loop(low, own + 1)
    def _(j):
        fetch(j).start()

    sums[...] = jnp.zeros_like(sums)
    total[...] = jnp.zeros_like(total)

    def gather(j, count, masked):
        for k in range(count):
            fetch(j + k).wait()
        keys = held[pl.ds(j, count), :, :HD].reshape(count * rows, HD)
        values = held[pl.ds(j, count), :, HD:].reshape(count * rows, HD)
        scores = lax.dot_general(
            query_ref[...], keys, (((1,), (1,)), ((), ())), preferred_element_type=jnp.float32
        )
        weights = jnp.exp(CAP * jnp.tanh(scores * (1.0 / CAP)))
        if masked:
            shape = (GROUP * rows, rows)
            row = lax.broadcasted_iota(jnp.int32, shape, 0)
            index = own * rows + jnp.where(row >= rows, row - rows, row)
            key_index = j * rows + lax.broadcasted_iota(jnp.int32, shape, 1)
            allowed = (key_index >= start_ref[...]) & (key_index <= index)
            weights = jnp.where(allowed, weights, 0.0)
        part = weights[:, :HD]
        for k in range(1, count * rows // HD):
            part = part + weights[:, k * HD : (k + 1) * HD]
        sums[...] += part
        total[...] += jnp.dot(
            weights.astype(jnp.bfloat16), values, preferred_element_type=jnp.float32
        )

    done = low + 1
    for count in (4, 2, 1):
        steps = lax.div(jnp.maximum(own - done, 0), count)

        @pl.loop(0, steps)
        def _(i, done=done, count=count):
            gather(done + i * count, count, False)

        done = done + steps * count

    seen = start_ref[...] < own * rows
    sums[...] = jnp.where(seen, sums[...], 0.0)
    total[...] = jnp.where(seen, total[...], 0.0)

    @pl.when(low < own)
    def _():
        gather(low, 1, True)

    gather(own, 1, True)

    result = total[...] / jnp.sum(sums[...], axis=1, keepdims=True)
    south = where_ref[3] == 0
    for k in range(GROUP):
        upper = result[k * rows : k * rows + rows // 2]
        lower = result[k * rows + rows // 2 : (k + 1) * rows]
        columns = slice(k * HD, (k + 1) * HD)
        near_ref[:, columns] = jnp.where(south, upper, lower).astype(jnp.bfloat16)
        away_ref[:, columns] = jnp.where(south, lower, upper).astype(jnp.bfloat16)


def attend(where, stacked, starts, kv):
    rows = stacked.shape[0] // GROUP
    blocks = kv.shape[0] // rows
    vmem = pl.BlockSpec(memory_space=pltpu.VMEM)
    return pl.pallas_call(
        attend_kernel,
        out_shape=[jax.ShapeDtypeStruct((rows // 2, GROUP * HD), jnp.bfloat16)] * 2,
        in_specs=[
            pl.BlockSpec(memory_space=pltpu.SMEM),
            vmem,
            vmem,
            pl.BlockSpec(memory_space=pltpu.HBM),
        ],
        out_specs=[vmem, vmem],
        scratch_shapes=[
            pltpu.VMEM((blocks, rows, 2 * HD), jnp.bfloat16),
            pltpu.VMEM((GROUP * rows, HD), jnp.float32),
            pltpu.VMEM((GROUP * rows, HD), jnp.float32),
            pltpu.SemaphoreType.DMA((blocks,)),
        ],
        compiler_params=pltpu.CompilerParams(vmem_limit_bytes=54 * 1024 * 1024),
        cost_estimate=pl.CostEstimate(
            flops=4 * GROUP * rows * HD * kv.shape[0] // 2,
            bytes_accessed=kv.size,
            transcendentals=GROUP * rows * kv.shape[0],
        ),
    )(where, stacked, starts, kv)


def finish_kernel(side_ref, part_ref, both_ref, cos_ref, sin_ref, out_ref):
    other = jnp.where(side_ref[0] == 0, both_ref[1], both_ref[0])
    keys = part_ref[:, :HD] + other[:, :HD].astype(jnp.float32)
    turned = keys * cos_ref[...] + pltpu.roll(keys, HD // 2, 1) * sin_ref[...]
    out_ref[:, :HD] = turned.astype(jnp.bfloat16)
    values = part_ref[:, HD:] + other[:, HD:].astype(jnp.float32)
    out_ref[:, HD:] = values.astype(jnp.bfloat16)


def finish(side, part, both, cosine, sine):
    vmem = pl.BlockSpec(memory_space=pltpu.VMEM)
    return pl.pallas_call(
        finish_kernel,
        out_shape=jax.ShapeDtypeStruct(part.shape, jnp.bfloat16),
        in_specs=[pl.BlockSpec(memory_space=pltpu.SMEM), vmem, vmem, vmem, vmem],
        out_specs=vmem,
        compiler_params=pltpu.CompilerParams(vmem_limit_bytes=16 * 1024 * 1024),
    )(side, part, both, cosine, sine)


def far_kernel(far_ref, near_ref, weight_hbm, out_ref, held, sem):
    pieces, width = held.shape[:2]

    def fetch(k):
        return pltpu.make_async_copy(
            weight_hbm.at[pl.ds(k * width, width), :], held.at[k], sem.at[k]
        )

    for k in range(pieces):
        fetch(k).start()
    for k in range(pieces):
        fetch(k).wait()
        columns = slice(k * width, (k + 1) * width)
        product = lax.dot_general(
            far_ref[...], held[k], (((1,), (1,)), ((), ())), preferred_element_type=jnp.float32
        )
        out_ref[:, columns] = (near_ref[:, columns] + product).astype(jnp.bfloat16)


def add_far(far, near_part, rows_of):
    pieces = 6
    vmem = pl.BlockSpec(memory_space=pltpu.VMEM)
    return pl.pallas_call(
        far_kernel,
        out_shape=jax.ShapeDtypeStruct(near_part.shape, jnp.bfloat16),
        in_specs=[vmem, vmem, pl.BlockSpec(memory_space=pltpu.HBM)],
        out_specs=vmem,
        scratch_shapes=[
            pltpu.VMEM((pieces, rows_of.shape[0] // pieces, rows_of.shape[1]), jnp.bfloat16),
            pltpu.SemaphoreType.DMA((pieces,)),
        ],
        compiler_params=pltpu.CompilerParams(vmem_limit_bytes=16 * 1024 * 1024),
    )(far, near_part, rows_of)


def local(tokens, segments, pre_gain, post_gain, w_query, w_key, w_value, w_out):
    rows, width = tokens.shape
    deep = lax.axis_size("z")
    mine = jnp.concatenate([w_key, w_value, w_query, w_out.T], axis=1)
    weights = lax.all_gather(mine, "z", axis=0, tiled=True)
    deep_half = weights.shape[0]

    ids = jnp.broadcast_to(segments.astype(jnp.bfloat16)[None, :], (16, rows))
    slices = jnp.concatenate([tokens.T, ids], axis=0)
    slices = lax.ppermute(slices, ("xh", "xl"), [(0, 0), (1, 2), (2, 1), (3, 3)])
    slices = from_everyone(slices[None], PLANE).reshape(-1, *slices.shape)
    slices = from_everyone(slices[None], "c").reshape(2, 2, -1, *slices.shape[1:])
    seg = slices[0, :, 0, width].astype(jnp.float32)
    levels = jnp.arange(DOCS, dtype=jnp.float32)
    counts = jnp.sum((levels[:, None, None] > seg[None]).astype(jnp.float32), axis=(1, 2))
    starts = jnp.sum(from_everyone(counts[None], "z").reshape(-1, DOCS), axis=0)
    onehot = (seg[:, :, None] == levels).astype(jnp.float32)
    tok_start = jnp.sum(onehot * starts, axis=2)
    side = lax.axis_index("xh")
    place = lax.axis_index("z")
    blocks = (jnp.arange(2, dtype=jnp.int32) * deep + place)[:, None] * rows
    index_f = (blocks + jnp.arange(rows, dtype=jnp.int32)).astype(jnp.float32)
    position = (index_f - tok_start).reshape(2 * rows)
    half = HD // 2
    freq = 10000.0 ** (-(jnp.arange(half, dtype=jnp.float32) / half))
    angle = position[:, None] * freq[None, :]
    cosine, sine = jnp.cos(angle), jnp.sin(angle)
    start_i = lax.dynamic_index_in_dim(tok_start, side, 0, keepdims=False).astype(jnp.int32)
    where = jnp.stack(
        [
            start_i[0] // rows,
            (side * deep + place).astype(jnp.int32),
            jnp.int32(deep),
            lax.axis_index("c").astype(jnp.int32),
        ]
    )
    starts_col = jnp.tile(start_i, GROUP)[:, None]

    wide = slices[:, :, :, :width].transpose(1, 2, 0, 3, 4).reshape(2, deep_half, rows)
    wide = wide.astype(jnp.float32)
    squares = jnp.sum(lax.all_gather(jnp.sum(wide * wide, axis=1), "xh", axis=0), axis=0)
    scale = lax.rsqrt(squares / D + EPS)
    gain = lax.dynamic_slice_in_dim(pre_gain, side * deep_half, deep_half, 0)
    normed = (wide * scale[:, None, :] * gain[None, :, None]).astype(jnp.bfloat16)
    normed = normed.transpose(0, 2, 1).reshape(2 * rows, deep_half)
    near = lax.axis_size(PLANE)
    few = rows // (near * 2)
    pieces = tokens.reshape(2, near, few, width).transpose(1, 0, 2, 3).reshape(-1, few, width)
    own = lax.all_to_all(pieces, HEAD, 0, 0, tiled=True).transpose(1, 0, 2).reshape(few, D)
    cos_wide = jnp.concatenate([cosine, cosine], axis=1)
    sin_wide = jnp.concatenate([-sine, sine], axis=1)
    normed, cosine, sine, cos_wide, sin_wide, weights, own = lax.optimization_barrier(
        (normed, cosine, sine, cos_wide, sin_wide, weights, own)
    )

    def project(columns):
        return jnp.dot(normed, columns, preferred_element_type=jnp.float32)

    part = project(weights[:, : 2 * HD])
    both = lax.all_gather(part.astype(jnp.bfloat16), "xh", axis=0)
    kv_pair = finish(side.astype(jnp.int32)[None], part, both, cos_wide, sin_wide)
    kv_pair, weights = lax.optimization_barrier((kv_pair, weights))
    kv_all = lax.all_gather(kv_pair, "z", axis=0, tiled=True)

    query = project(weights[:, 2 * HD : 4 * HD]).reshape(2, rows, 2 * HD)
    query = jnp.sum(lax.all_to_all(query, "xh", 0, 0, tiled=True), axis=0)
    own_cos = lax.dynamic_slice_in_dim(cosine, side * rows, rows, 0)
    own_sin = lax.dynamic_slice_in_dim(sine, side * rows, rows, 0)
    stacked = jnp.concatenate(
        [
            (rotate(query[:, k * HD : (k + 1) * HD], own_cos, own_sin) * SCALAR ** (-0.5)).astype(
                jnp.bfloat16
            )
            for k in range(GROUP)
        ],
        axis=0,
    )
    out_t = from_everyone(weights[None, :, 4 * HD :], "xh").reshape(D, GROUP * HD)
    swap = [(0, 1), (1, 0)]
    out_far = lax.ppermute(out_t, "c", swap)
    kv_all, stacked, out_t, out_far = lax.optimization_barrier((kv_all, stacked, out_t, out_far))

    kept, away = attend(where, stacked, starts_col, kv_all)
    far = lax.ppermute(away, "c", swap)

    def through(part, rows_of):
        return lax.dot_general(
            part, rows_of, (((1,), (1,)), ((), ())), preferred_element_type=jnp.float32
        )

    near_part = through(kept, out_t)
    near_part, far = lax.optimization_barrier((near_part, far))
    halves = add_far(far, near_part, out_far)
    pieces = lax.all_to_all(halves.reshape(near, few, D), PLANE, 0, 0, tiled=True)
    proj = jnp.sum(pieces.astype(jnp.float32), axis=0)
    post = lax.rsqrt(jnp.mean(proj * proj, axis=1, keepdims=True) + EPS)
    result = (own.astype(jnp.float32) + proj * post * post_gain[None, :]).astype(jnp.bfloat16)
    result = from_everyone(result, PLANE).reshape(rows // 2, D)
    other = lax.ppermute(result, "c", swap)
    mine_first = (jnp.arange(2) == lax.axis_index("c"))[:, None, None]
    return jnp.where(mine_first, result[None], other[None]).reshape(rows, D)


def solution(mesh):
    finer = Mesh(mesh.devices.reshape(2, 16, 2, 4, 2), ("xh", "z", "xl", "y", "c"))
    in_specs = (
        P(SEQ, HEAD),
        P(SEQ),
        P(),
        P(),
        P(SEQ, HEAD),
        P(SEQ, HEAD),
        P(SEQ, HEAD),
        P(HEAD, SEQ),
    )
    return jax.shard_map(
        local, mesh=finer, in_specs=in_specs, out_specs=P(SEQ, None), check_vma=False
    )
```

```python
import jax
import jax.numpy as jnp
from jax import lax
from jax.experimental import pallas as pl
from jax.experimental.pallas import tpu as pltpu
from jax.sharding import Mesh
from jax.sharding import PartitionSpec as P

D = 4608
HD = 128
GROUP = 2
SCALAR = 144
DOCS = 8
SEQ = ("xh", "z")
HEAD = ("xl", "y", "c")
PLANE = ("xl", "y")

EPS = 1e-06
CAP = 50.0


def from_everyone(shard, axis):
    copies = jnp.broadcast_to(shard, (lax.axis_size(axis), *shard.shape))
    return lax.all_to_all(copies, axis, split_axis=0, concat_axis=0, tiled=True)


def rotate(values, cosine, sine):
    half = values.shape[1] // 2
    first = values[:, :half]
    second = values[:, half:]
    return jnp.concatenate(
        [first * cosine - second * sine, second * cosine + first * sine], axis=1
    )


def attend_kernel(
    where_ref, query_ref, start_ref, kv_hbm, near_ref, away_ref, held, sums, total, sem
):
    rows = query_ref.shape[0] // GROUP
    low = where_ref[0]
    own = where_ref[1]
    halves = where_ref[2]

    def fetch(j):
        place = (lax.rem(j, halves) * 2 + lax.div(j, halves)) * rows
        return pltpu.make_async_copy(
            kv_hbm.at[pl.ds(pl.multiple_of(place, rows), rows), :], held.at[j], sem.at[j]
        )

    @pl.loop(low, own + 1)
    def _(j):
        fetch(j).start()

    sums[...] = jnp.zeros_like(sums)
    total[...] = jnp.zeros_like(total)

    def weigh(keys):
        scores = lax.dot_general(
            query_ref[...], keys, (((1,), (1,)), ((), ())), preferred_element_type=jnp.float32
        )
        return jnp.exp(CAP * jnp.tanh(scores * (1.0 / CAP)))

    def add(weights, values):
        part = weights[:, :HD]
        for k in range(1, weights.shape[1] // HD):
            part = part + weights[:, k * HD : (k + 1) * HD]
        sums[...] += part
        total[...] += jnp.dot(
            weights.astype(jnp.bfloat16), values, preferred_element_type=jnp.float32
        )

    def gather(j, count):
        for k in range(count):
            fetch(j + k).wait()
        keys = held[pl.ds(j, count), :, :HD].reshape(count * rows, HD)
        values = held[pl.ds(j, count), :, HD:].reshape(count * rows, HD)
        add(weigh(keys), values)

    done = low + 1
    for count in (4, 2, 1):
        steps = lax.div(jnp.maximum(own - done, 0), count)

        @pl.loop(0, steps)
        def _(i, done=done, count=count):
            gather(done + i * count, count)

        done = done + steps * count

    seen = start_ref[...] < own * rows
    sums[...] = jnp.where(seen, sums[...], 0.0)
    total[...] = jnp.where(seen, total[...], 0.0)

    @pl.when(low < own)
    def _():
        fetch(low).wait()

    fetch(own).wait()
    weights = weigh(jnp.concatenate([held[low, :, :HD], held[own, :, :HD]], axis=0))
    shape = (GROUP * rows, rows)
    row = lax.broadcasted_iota(jnp.int32, shape, 0)
    row = jnp.where(row >= rows, row - rows, row)
    column = lax.broadcasted_iota(jnp.int32, shape, 1)
    edge = jnp.where(low < own, low * rows, -rows)
    early = jnp.where(edge + column >= start_ref[...], weights[:, :rows], 0.0)
    late = (own * rows + column >= start_ref[...]) & (column <= row)
    late = jnp.where(late, weights[:, rows:], 0.0)
    add(
        jnp.concatenate([early, late], axis=1),
        jnp.concatenate([held[low, :, HD:], held[own, :, HD:]], axis=0),
    )

    result = total[...] / jnp.sum(sums[...], axis=1, keepdims=True)
    south = where_ref[3] == 0
    for k in range(GROUP):
        upper = result[k * rows : k * rows + rows // 2]
        lower = result[k * rows + rows // 2 : (k + 1) * rows]
        columns = slice(k * HD, (k + 1) * HD)
        near_ref[:, columns] = jnp.where(south, upper, lower).astype(jnp.bfloat16)
        away_ref[:, columns] = jnp.where(south, lower, upper).astype(jnp.bfloat16)


def attend(where, stacked, starts, kv):
    rows = stacked.shape[0] // GROUP
    blocks = kv.shape[0] // rows
    vmem = pl.BlockSpec(memory_space=pltpu.VMEM)
    return pl.pallas_call(
        attend_kernel,
        out_shape=[jax.ShapeDtypeStruct((rows // 2, GROUP * HD), jnp.bfloat16)] * 2,
        in_specs=[
            pl.BlockSpec(memory_space=pltpu.SMEM),
            vmem,
            vmem,
            pl.BlockSpec(memory_space=pltpu.HBM),
        ],
        out_specs=[vmem, vmem],
        scratch_shapes=[
            pltpu.VMEM((blocks, rows, 2 * HD), jnp.bfloat16),
            pltpu.VMEM((GROUP * rows, HD), jnp.float32),
            pltpu.VMEM((GROUP * rows, HD), jnp.float32),
            pltpu.SemaphoreType.DMA((blocks,)),
        ],
        compiler_params=pltpu.CompilerParams(vmem_limit_bytes=54 * 1024 * 1024),
        cost_estimate=pl.CostEstimate(
            flops=4 * GROUP * rows * HD * kv.shape[0] // 2,
            bytes_accessed=kv.size,
            transcendentals=GROUP * rows * kv.shape[0],
        ),
    )(where, stacked, starts, kv)


def finish_kernel(side_ref, part_ref, both_ref, cos_ref, sin_ref, out_ref):
    other = jnp.where(side_ref[0] == 0, both_ref[1], both_ref[0])
    keys = part_ref[:, :HD] + other[:, :HD].astype(jnp.float32)
    turned = keys * cos_ref[...] + pltpu.roll(keys, HD // 2, 1) * sin_ref[...]
    out_ref[:, :HD] = turned.astype(jnp.bfloat16)
    values = part_ref[:, HD:] + other[:, HD:].astype(jnp.float32)
    out_ref[:, HD:] = values.astype(jnp.bfloat16)


def finish(side, part, both, cosine, sine):
    vmem = pl.BlockSpec(memory_space=pltpu.VMEM)
    return pl.pallas_call(
        finish_kernel,
        out_shape=jax.ShapeDtypeStruct(part.shape, jnp.bfloat16),
        in_specs=[pl.BlockSpec(memory_space=pltpu.SMEM), vmem, vmem, vmem, vmem],
        out_specs=vmem,
        compiler_params=pltpu.CompilerParams(vmem_limit_bytes=16 * 1024 * 1024),
    )(side, part, both, cosine, sine)


def local(tokens, segments, pre_gain, post_gain, w_query, w_key, w_value, w_out):
    rows, width = tokens.shape
    deep = lax.axis_size("z")
    mine = jnp.concatenate([w_key, w_value, w_query, w_out.T], axis=1)
    weights = lax.all_gather(mine, "z", axis=0, tiled=True)
    deep_half = weights.shape[0]

    ids = jnp.broadcast_to(segments.astype(jnp.bfloat16)[None, :], (16, rows))
    slices = jnp.concatenate([tokens.T, ids], axis=0)
    slices = lax.ppermute(slices, ("xh", "xl"), [(0, 0), (1, 2), (2, 1), (3, 3)])
    slices = from_everyone(slices[None], PLANE).reshape(-1, *slices.shape)
    slices = from_everyone(slices[None], "c").reshape(2, 2, -1, *slices.shape[1:])
    seg = slices[0, :, 0, width].astype(jnp.float32)
    levels = jnp.arange(DOCS, dtype=jnp.float32)
    counts = jnp.sum((levels[:, None, None] > seg[None]).astype(jnp.float32), axis=(1, 2))
    starts = jnp.sum(from_everyone(counts[None], "z").reshape(-1, DOCS), axis=0)
    onehot = (seg[:, :, None] == levels).astype(jnp.float32)
    tok_start = jnp.sum(onehot * starts, axis=2)
    side = lax.axis_index("xh")
    place = lax.axis_index("z")
    blocks = (jnp.arange(2, dtype=jnp.int32) * deep + place)[:, None] * rows
    index_f = (blocks + jnp.arange(rows, dtype=jnp.int32)).astype(jnp.float32)
    position = (index_f - tok_start).reshape(2 * rows)
    half = HD // 2
    freq = 10000.0 ** (-(jnp.arange(half, dtype=jnp.float32) / half))
    angle = position[:, None] * freq[None, :]
    cosine, sine = jnp.cos(angle), jnp.sin(angle)
    start_i = lax.dynamic_index_in_dim(tok_start, side, 0, keepdims=False).astype(jnp.int32)
    where = jnp.stack(
        [
            start_i[0] // rows,
            (side * deep + place).astype(jnp.int32),
            jnp.int32(deep),
            lax.axis_index("c").astype(jnp.int32),
        ]
    )
    starts_col = jnp.tile(start_i, GROUP)[:, None]

    wide = slices[:, :, :, :width].transpose(1, 2, 0, 3, 4).reshape(2, deep_half, rows)
    wide = wide.astype(jnp.float32)
    squares = jnp.sum(lax.all_gather(jnp.sum(wide * wide, axis=1), "xh", axis=0), axis=0)
    scale = lax.rsqrt(squares / D + EPS)
    gain = lax.dynamic_slice_in_dim(pre_gain, side * deep_half, deep_half, 0)
    normed = (wide * scale[:, None, :] * gain[None, :, None]).astype(jnp.bfloat16)
    normed = normed.transpose(0, 2, 1).reshape(2 * rows, deep_half)
    near = lax.axis_size(PLANE)
    few = rows // (near * 2)
    pieces = tokens.reshape(2, near, few, width).transpose(1, 0, 2, 3).reshape(-1, few, width)
    own = lax.all_to_all(pieces, HEAD, 0, 0, tiled=True).transpose(1, 0, 2).reshape(few, D)
    cos_wide = jnp.concatenate([cosine, cosine], axis=1)
    sin_wide = jnp.concatenate([-sine, sine], axis=1)
    normed, cosine, sine, cos_wide, sin_wide, weights, own = lax.optimization_barrier(
        (normed, cosine, sine, cos_wide, sin_wide, weights, own)
    )

    def project(columns):
        return jnp.dot(normed, columns, preferred_element_type=jnp.float32)

    part = project(weights[:, : 2 * HD])
    both = lax.all_gather(part.astype(jnp.bfloat16), "xh", axis=0)
    kv_pair = finish(side.astype(jnp.int32)[None], part, both, cos_wide, sin_wide)
    kv_pair, weights = lax.optimization_barrier((kv_pair, weights))
    kv_all = lax.all_gather(kv_pair, "z", axis=0, tiled=True)

    query = project(weights[:, 2 * HD : 4 * HD]).reshape(2, rows, 2 * HD)
    query = jnp.sum(lax.all_to_all(query, "xh", 0, 0, tiled=True), axis=0)
    own_cos = lax.dynamic_slice_in_dim(cosine, side * rows, rows, 0)
    own_sin = lax.dynamic_slice_in_dim(sine, side * rows, rows, 0)
    stacked = jnp.concatenate(
        [
            (rotate(query[:, k * HD : (k + 1) * HD], own_cos, own_sin) * SCALAR ** (-0.5)).astype(
                jnp.bfloat16
            )
            for k in range(GROUP)
        ],
        axis=0,
    )
    out_t = from_everyone(weights[None, :, 4 * HD :], "xh").reshape(D, GROUP * HD)
    swap = [(0, 1), (1, 0)]
    out_far = lax.ppermute(out_t, "c", swap)
    kv_all, stacked, out_t, out_far = lax.optimization_barrier((kv_all, stacked, out_t, out_far))

    kept, away = attend(where, stacked, starts_col, kv_all)
    far = lax.ppermute(away, "c", swap)

    def through(part, rows_of):
        return lax.dot_general(
            part, rows_of, (((1,), (1,)), ((), ())), preferred_element_type=jnp.float32
        )

    near_part = through(kept, out_t)
    near_part, far = lax.optimization_barrier((near_part, far))
    halves = (near_part + through(far, out_far)).astype(jnp.bfloat16)
    pieces = lax.all_to_all(halves.reshape(near, few, D), PLANE, 0, 0, tiled=True)
    proj = jnp.sum(pieces.astype(jnp.float32), axis=0)
    post = lax.rsqrt(jnp.mean(proj * proj, axis=1, keepdims=True) + EPS)
    result = (own.astype(jnp.float32) + proj * post * post_gain[None, :]).astype(jnp.bfloat16)
    result = from_everyone(result, PLANE).reshape(rows // 2, D)
    other = lax.ppermute(result, "c", swap)
    mine_first = (jnp.arange(2) == lax.axis_index("c"))[:, None, None]
    return jnp.where(mine_first, result[None], other[None]).reshape(rows, D)


def solution(mesh):
    finer = Mesh(mesh.devices.reshape(2, 16, 2, 4, 2), ("xh", "z", "xl", "y", "c"))
    in_specs = (
        P(SEQ, HEAD),
        P(SEQ),
        P(),
        P(),
        P(SEQ, HEAD),
        P(SEQ, HEAD),
        P(SEQ, HEAD),
        P(HEAD, SEQ),
    )
    return jax.shard_map(
        local, mesh=finer, in_specs=in_specs, out_specs=P(SEQ, None), check_vma=False
    )
```

```python
import jax
import jax.numpy as jnp
from jax import lax
from jax.experimental import pallas as pl
from jax.experimental.pallas import tpu as pltpu
from jax.sharding import Mesh
from jax.sharding import PartitionSpec as P

D = 4608
HD = 128
GROUP = 2
SCALAR = 144
DOCS = 8
SEQ = ("xh", "z")
HEAD = ("xl", "y", "c")
PLANE = ("xl", "y")

EPS = 1e-06
CAP = 50.0


def from_everyone(shard, axis):
    copies = jnp.broadcast_to(shard, (lax.axis_size(axis), *shard.shape))
    return lax.all_to_all(copies, axis, split_axis=0, concat_axis=0, tiled=True)


def rotate(values, cosine, sine):
    half = values.shape[1] // 2
    first = values[:, :half]
    second = values[:, half:]
    return jnp.concatenate(
        [first * cosine - second * sine, second * cosine + first * sine], axis=1
    )


def attend_kernel(
    where_ref, query_ref, start_ref, kv_hbm, near_ref, away_ref, held, sums, total, sem
):
    rows = query_ref.shape[0] // GROUP
    low = where_ref[0]
    own = where_ref[1]
    halves = where_ref[2]

    def fetch(j):
        place = (lax.rem(j, halves) * 2 + lax.div(j, halves)) * rows
        return pltpu.make_async_copy(
            kv_hbm.at[pl.ds(pl.multiple_of(place, rows), rows), :], held.at[j], sem.at[j]
        )

    @pl.loop(low, own + 1)
    def _(j):
        fetch(j).start()

    sums[...] = jnp.zeros_like(sums)
    total[...] = jnp.zeros_like(total)

    def weigh(keys):
        scores = lax.dot_general(
            query_ref[...], keys, (((1,), (1,)), ((), ())), preferred_element_type=jnp.float32
        )
        return jnp.exp(CAP * jnp.tanh(scores * (1.0 / CAP)))

    def add(weights, values):
        part = weights[:, :HD]
        for k in range(1, weights.shape[1] // HD):
            part = part + weights[:, k * HD : (k + 1) * HD]
        sums[...] += part
        total[...] += jnp.dot(
            weights.astype(jnp.bfloat16), values, preferred_element_type=jnp.float32
        )

    def gather(j, count):
        for k in range(count):
            fetch(j + k).wait()
        keys = held[pl.ds(j, count), :, :HD].reshape(count * rows, HD)
        values = held[pl.ds(j, count), :, HD:].reshape(count * rows, HD)
        add(weigh(keys), values)

    done = low + 1
    for count in (5, 2, 1):
        steps = lax.div(jnp.maximum(own - done, 0), count)

        @pl.loop(0, steps)
        def _(i, done=done, count=count):
            gather(done + i * count, count)

        done = done + steps * count

    seen = start_ref[...] < own * rows
    sums[...] = jnp.where(seen, sums[...], 0.0)
    total[...] = jnp.where(seen, total[...], 0.0)

    @pl.when(low < own)
    def _():
        fetch(low).wait()

    fetch(own).wait()
    weights = weigh(jnp.concatenate([held[low, :, :HD], held[own, :, :HD]], axis=0))
    shape = (GROUP * rows, rows)
    row = lax.broadcasted_iota(jnp.int32, shape, 0)
    row = jnp.where(row >= rows, row - rows, row)
    column = lax.broadcasted_iota(jnp.int32, shape, 1)
    edge = jnp.where(low < own, low * rows, -rows)
    early = jnp.where(edge + column >= start_ref[...], weights[:, :rows], 0.0)
    late = (own * rows + column >= start_ref[...]) & (column <= row)
    late = jnp.where(late, weights[:, rows:], 0.0)
    add(
        jnp.concatenate([early, late], axis=1),
        jnp.concatenate([held[low, :, HD:], held[own, :, HD:]], axis=0),
    )

    result = total[...] / jnp.sum(sums[...], axis=1, keepdims=True)
    south = where_ref[3] == 0
    for k in range(GROUP):
        upper = result[k * rows : k * rows + rows // 2]
        lower = result[k * rows + rows // 2 : (k + 1) * rows]
        columns = slice(k * HD, (k + 1) * HD)
        near_ref[:, columns] = jnp.where(south, upper, lower).astype(jnp.bfloat16)
        away_ref[:, columns] = jnp.where(south, lower, upper).astype(jnp.bfloat16)


def attend(where, stacked, starts, kv):
    rows = stacked.shape[0] // GROUP
    blocks = kv.shape[0] // rows
    vmem = pl.BlockSpec(memory_space=pltpu.VMEM)
    return pl.pallas_call(
        attend_kernel,
        out_shape=[jax.ShapeDtypeStruct((rows // 2, GROUP * HD), jnp.bfloat16)] * 2,
        in_specs=[
            pl.BlockSpec(memory_space=pltpu.SMEM),
            vmem,
            vmem,
            pl.BlockSpec(memory_space=pltpu.HBM),
        ],
        out_specs=[vmem, vmem],
        scratch_shapes=[
            pltpu.VMEM((blocks, rows, 2 * HD), jnp.bfloat16),
            pltpu.VMEM((GROUP * rows, HD), jnp.float32),
            pltpu.VMEM((GROUP * rows, HD), jnp.float32),
            pltpu.SemaphoreType.DMA((blocks,)),
        ],
        compiler_params=pltpu.CompilerParams(vmem_limit_bytes=54 * 1024 * 1024),
        cost_estimate=pl.CostEstimate(
            flops=4 * GROUP * rows * HD * kv.shape[0] // 2,
            bytes_accessed=kv.size,
            transcendentals=GROUP * rows * kv.shape[0],
        ),
    )(where, stacked, starts, kv)


def finish_kernel(side_ref, part_ref, both_ref, cos_ref, sin_ref, out_ref):
    other = jnp.where(side_ref[0] == 0, both_ref[1], both_ref[0])
    keys = part_ref[:, :HD] + other[:, :HD].astype(jnp.float32)
    turned = keys * cos_ref[...] + pltpu.roll(keys, HD // 2, 1) * sin_ref[...]
    out_ref[:, :HD] = turned.astype(jnp.bfloat16)
    values = part_ref[:, HD:] + other[:, HD:].astype(jnp.float32)
    out_ref[:, HD:] = values.astype(jnp.bfloat16)


def finish(side, part, both, cosine, sine):
    vmem = pl.BlockSpec(memory_space=pltpu.VMEM)
    return pl.pallas_call(
        finish_kernel,
        out_shape=jax.ShapeDtypeStruct(part.shape, jnp.bfloat16),
        in_specs=[pl.BlockSpec(memory_space=pltpu.SMEM), vmem, vmem, vmem, vmem],
        out_specs=vmem,
        compiler_params=pltpu.CompilerParams(vmem_limit_bytes=16 * 1024 * 1024),
    )(side, part, both, cosine, sine)


def local(tokens, segments, pre_gain, post_gain, w_query, w_key, w_value, w_out):
    rows, width = tokens.shape
    deep = lax.axis_size("z")
    mine = jnp.concatenate([w_key, w_value, w_query, w_out.T], axis=1)
    weights = lax.all_gather(mine, "z", axis=0, tiled=True)
    deep_half = weights.shape[0]

    ids = jnp.broadcast_to(segments.astype(jnp.bfloat16)[None, :], (16, rows))
    slices = jnp.concatenate([tokens.T, ids], axis=0)
    slices = lax.ppermute(slices, ("xh", "xl"), [(0, 0), (1, 2), (2, 1), (3, 3)])
    slices = from_everyone(slices[None], PLANE).reshape(-1, *slices.shape)
    slices = from_everyone(slices[None], "c").reshape(2, 2, -1, *slices.shape[1:])
    seg = slices[0, :, 0, width].astype(jnp.float32)
    levels = jnp.arange(DOCS, dtype=jnp.float32)
    counts = jnp.sum((levels[:, None, None] > seg[None]).astype(jnp.float32), axis=(1, 2))
    starts = jnp.sum(from_everyone(counts[None], "z").reshape(-1, DOCS), axis=0)
    onehot = (seg[:, :, None] == levels).astype(jnp.float32)
    tok_start = jnp.sum(onehot * starts, axis=2)
    side = lax.axis_index("xh")
    place = lax.axis_index("z")
    blocks = (jnp.arange(2, dtype=jnp.int32) * deep + place)[:, None] * rows
    index_f = (blocks + jnp.arange(rows, dtype=jnp.int32)).astype(jnp.float32)
    position = (index_f - tok_start).reshape(2 * rows)
    half = HD // 2
    freq = 10000.0 ** (-(jnp.arange(half, dtype=jnp.float32) / half))
    angle = position[:, None] * freq[None, :]
    cosine, sine = jnp.cos(angle), jnp.sin(angle)
    start_i = lax.dynamic_index_in_dim(tok_start, side, 0, keepdims=False).astype(jnp.int32)
    where = jnp.stack(
        [
            start_i[0] // rows,
            (side * deep + place).astype(jnp.int32),
            jnp.int32(deep),
            lax.axis_index("c").astype(jnp.int32),
        ]
    )
    starts_col = jnp.tile(start_i, GROUP)[:, None]

    wide = slices[:, :, :, :width].transpose(1, 2, 0, 3, 4).reshape(2, deep_half, rows)
    wide = wide.astype(jnp.float32)
    squares = jnp.sum(lax.all_gather(jnp.sum(wide * wide, axis=1), "xh", axis=0), axis=0)
    scale = lax.rsqrt(squares / D + EPS)
    gain = lax.dynamic_slice_in_dim(pre_gain, side * deep_half, deep_half, 0)
    normed = (wide * scale[:, None, :] * gain[None, :, None]).astype(jnp.bfloat16)
    normed = normed.transpose(0, 2, 1).reshape(2 * rows, deep_half)
    near = lax.axis_size(PLANE)
    few = rows // (near * 2)
    pieces = tokens.reshape(2, near, few, width).transpose(1, 0, 2, 3).reshape(-1, few, width)
    own = lax.all_to_all(pieces, HEAD, 0, 0, tiled=True).transpose(1, 0, 2).reshape(few, D)
    cos_wide = jnp.concatenate([cosine, cosine], axis=1)
    sin_wide = jnp.concatenate([-sine, sine], axis=1)
    normed, cosine, sine, cos_wide, sin_wide, weights, own = lax.optimization_barrier(
        (normed, cosine, sine, cos_wide, sin_wide, weights, own)
    )

    def project(columns):
        return jnp.dot(normed, columns, preferred_element_type=jnp.float32)

    part = project(weights[:, : 2 * HD])
    both = lax.all_gather(part.astype(jnp.bfloat16), "xh", axis=0)
    kv_pair = finish(side.astype(jnp.int32)[None], part, both, cos_wide, sin_wide)
    kv_pair, weights = lax.optimization_barrier((kv_pair, weights))
    kv_all = lax.all_gather(kv_pair, "z", axis=0, tiled=True)

    query = project(weights[:, 2 * HD : 4 * HD]).reshape(2, rows, 2 * HD)
    query = jnp.sum(lax.all_to_all(query, "xh", 0, 0, tiled=True), axis=0)
    own_cos = lax.dynamic_slice_in_dim(cosine, side * rows, rows, 0)
    own_sin = lax.dynamic_slice_in_dim(sine, side * rows, rows, 0)
    stacked = jnp.concatenate(
        [
            (rotate(query[:, k * HD : (k + 1) * HD], own_cos, own_sin) * SCALAR ** (-0.5)).astype(
                jnp.bfloat16
            )
            for k in range(GROUP)
        ],
        axis=0,
    )
    out_t = from_everyone(weights[None, :, 4 * HD :], "xh").reshape(D, GROUP * HD)
    swap = [(0, 1), (1, 0)]
    out_far = lax.ppermute(out_t, "c", swap)
    kv_all, stacked, out_t, out_far = lax.optimization_barrier((kv_all, stacked, out_t, out_far))

    kept, away = attend(where, stacked, starts_col, kv_all)
    far = lax.ppermute(away, "c", swap)

    def through(part, rows_of):
        return lax.dot_general(
            part, rows_of, (((1,), (1,)), ((), ())), preferred_element_type=jnp.float32
        )

    near_part = through(kept, out_t)
    near_part, far = lax.optimization_barrier((near_part, far))
    halves = (near_part + through(far, out_far)).astype(jnp.bfloat16)
    pieces = lax.all_to_all(halves.reshape(near, few, D), PLANE, 0, 0, tiled=True)
    proj = jnp.sum(pieces.astype(jnp.float32), axis=0)
    post = lax.rsqrt(jnp.mean(proj * proj, axis=1, keepdims=True) + EPS)
    result = (own.astype(jnp.float32) + proj * post * post_gain[None, :]).astype(jnp.bfloat16)
    result = from_everyone(result, PLANE).reshape(rows // 2, D)
    other = lax.ppermute(result, "c", swap)
    mine_first = (jnp.arange(2) == lax.axis_index("c"))[:, None, None]
    return jnp.where(mine_first, result[None], other[None]).reshape(rows, D)


def solution(mesh):
    finer = Mesh(mesh.devices.reshape(2, 16, 2, 4, 2), ("xh", "z", "xl", "y", "c"))
    in_specs = (
        P(SEQ, HEAD),
        P(SEQ),
        P(),
        P(),
        P(SEQ, HEAD),
        P(SEQ, HEAD),
        P(SEQ, HEAD),
        P(HEAD, SEQ),
    )
    return jax.shard_map(
        local, mesh=finer, in_specs=in_specs, out_specs=P(SEQ, None), check_vma=False
    )
```
